128 devices in a mesh: data: 128 (over z, y, x, core).
Axes of the slice: x: 4, y: 4, z: 4, core: 2. Of those that a mesh axis runs over, the one named last changes fastest.
Arguments:
- x_step: bfloat16 [2, 256, 196, 512], P(None, 'data')
- labels: int32 [2, 256], P(None, 'data')
- x_next: bfloat16 [256, 196, 512], P('data')
- w_in: float32 [6, 512, 2048], replicated
- w_out: float32 [6, 2048, 512], replicated
- w_head: float32 [512, 1000], replicated
- mom_in: float32 [6, 512, 2048], replicated
- mom_out: float32 [6, 2048, 512], replicated
- mom_head: float32 [512, 1000], replicated
- learn_rate: float32 [], replicated
- mom_coef: float32 [], replicated
Outputs:
- output 1: float32 [256, 1000], P('data')
- output 2: float32 [6, 512, 2048], replicated
- output 3: float32 [6, 2048, 512], replicated
- output 4: float32 [512, 1000], replicated
- output 5: float32 [6, 512, 2048], replicated
- output 6: float32 [6, 2048, 512], replicated
- output 7: float32 [512, 1000], replicated
All inputs are finite; a program needn't handle non-finite values.
Results may differ from the reference program's by a relative error of at most 0.0168491.
Values are sent between devices in bfloat16 or wider.
A program may use at most 1 GiB of HBM per device.

```python
import jax
import jax.numpy as jnp
from jax import lax

D = 512
FF = 2048
SEQ = 196
CLASSES = 1000
LAYERS = 6
BATCH_DEV = 2
GROUP = 128
MICRO = 2
BATCH = GROUP * BATCH_DEV
EXAMPLES = MICRO * BATCH
LN_EPS = 1e-6


def setup_inputs(seed: int = 0) -> dict:
    key_list = jax.random.split(jax.random.key(seed), 13)
    img_step = jax.random.normal(key_list[0], (MICRO, BATCH, 1, D), jnp.float32)
    tok_step = jax.random.normal(key_list[1], (MICRO, BATCH, SEQ, D), jnp.float32)
    img_next = jax.random.normal(key_list[2], (BATCH, 1, D), jnp.float32)
    tok_next = jax.random.normal(key_list[3], (BATCH, SEQ, D), jnp.float32)
    labels = jax.random.randint(key_list[4], (MICRO, BATCH), 0, CLASSES, jnp.int32)
    in_scale = D ** -0.5
    out_scale = FF ** -0.5
    mom_rel = 0.3 * EXAMPLES ** -0.5
    return {
        'x_step': (0.8 * img_step + 0.6 * tok_step).astype(jnp.bfloat16),
        'labels': labels,
        'x_next': (0.8 * img_next + 0.6 * tok_next).astype(jnp.bfloat16),
        'w_in': jax.random.normal(key_list[5], (LAYERS, D, FF), jnp.float32) * in_scale,
        'w_out': jax.random.normal(key_list[6], (LAYERS, FF, D), jnp.float32) * out_scale,
        'w_head': jax.random.normal(key_list[7], (D, CLASSES), jnp.float32) * in_scale,
        'mom_in': jax.random.normal(key_list[8], (LAYERS, D, FF), jnp.float32) * (in_scale * mom_rel),
        'mom_out': jax.random.normal(key_list[9], (LAYERS, FF, D), jnp.float32) * (out_scale * mom_rel),
        'mom_head': jax.random.normal(key_list[10], (D, CLASSES), jnp.float32) * (in_scale * mom_rel),
        'learn_rate': jax.random.uniform(key_list[11], (), jnp.float32, 0.1, 0.2) * EXAMPLES ** 0.5,
        'mom_coef': jax.random.uniform(key_list[12], (), jnp.float32, 0.5, 0.9),
    }


def norm_rows(x_f32):
    row_mean = jnp.mean(x_f32, axis=-1, keepdims=True)
    centered = x_f32 - row_mean
    row_var = jnp.mean(centered * centered, axis=-1, keepdims=True)
    return centered * lax.rsqrt(row_var + LN_EPS)


def block_forward(tok_rows, w_one, w_two):
    x_f32 = tok_rows.astype(jnp.float32)
    normed = norm_rows(x_f32).astype(jnp.bfloat16)
    pre_act = jnp.dot(normed, w_one.astype(jnp.bfloat16), preferred_element_type=jnp.float32)
    hidden = jax.nn.gelu(pre_act).astype(jnp.bfloat16)
    mlp_out = jnp.dot(hidden, w_two.astype(jnp.bfloat16), preferred_element_type=jnp.float32)
    return (x_f32 + mlp_out).astype(jnp.bfloat16)


def image_logits(images, w_in, w_out, w_head):
    n_img = images.shape[0]

    def layer_step(tok_rows, weights):
        return block_forward(tok_rows, weights[0], weights[1]), None

    tok_rows, _ = lax.scan(layer_step, images.reshape(n_img * SEQ, D), (w_in, w_out))
    pooled = jnp.mean(tok_rows.reshape(n_img, SEQ, D), axis=1, dtype=jnp.float32)
    return jnp.dot(pooled.astype(jnp.bfloat16), w_head.astype(jnp.bfloat16), preferred_element_type=jnp.float32)


def group_loss(params, images, lab_row):
    logits = image_logits(images, params[0], params[1], params[2])
    log_prob = jax.nn.log_softmax(logits, axis=-1)
    picked = jnp.take_along_axis(log_prob, lab_row[:, None], axis=-1)
    return -jnp.sum(picked) / EXAMPLES


def reference(x_step, labels, x_next, w_in, w_out, w_head, mom_in, mom_out, mom_head, learn_rate, mom_coef):
    params = (w_in, w_out, w_head)
    img_groups = x_step.reshape(MICRO * GROUP, BATCH_DEV, SEQ, D)
    lab_groups = labels.reshape(MICRO * GROUP, BATCH_DEV)
    grad_fn = jax.grad(group_loss)

    def accumulate(grad_sum, group_in):
        part_grad = grad_fn(params, group_in[0], group_in[1])
        return jax.tree.map(jnp.add, grad_sum, part_grad), None

    zero_grads = jax.tree.map(jnp.zeros_like, params)
    grad_sum, _ = lax.scan(accumulate, zero_grads, (img_groups, lab_groups))
    new_mom_in = mom_coef * mom_in + grad_sum[0]
    new_mom_out = mom_coef * mom_out + grad_sum[1]
    new_mom_head = mom_coef * mom_head + grad_sum[2]
    new_w_in = w_in - learn_rate * new_mom_in
    new_w_out = w_out - learn_rate * new_mom_out
    new_w_head = w_head - learn_rate * new_mom_head
    next_groups = x_next.reshape(GROUP, BATCH_DEV, SEQ, D)
    logits = lax.map(lambda images: image_logits(images, new_w_in, new_w_out, new_w_head), next_groups)
    return (logits.reshape(BATCH, CLASSES), new_w_in, new_w_out, new_w_head, new_mom_in, new_mom_out, new_mom_head)
```

```python
import functools

import jax
import jax.numpy as jnp
from jax import lax
from jax.experimental import pallas as pl
from jax.experimental.pallas import tpu as pltpu
from jax.sharding import PartitionSpec as P

LN_EPS = 1e-6
GELU_A = 0.7978845608028654
GELU_B = 0.044715
CHUNK = 512
LANES = 256
MESH_ID = pl.DeviceIdType.MESH
F32 = jnp.float32
BF16 = jnp.bfloat16


def norm_parts(x_f32):
    row_mean = jnp.mean(x_f32, axis=-1, keepdims=True)
    centered = x_f32 - row_mean
    row_var = jnp.mean(centered * centered, axis=-1, keepdims=True)
    inv = lax.rsqrt(row_var + LN_EPS)
    return centered * inv, inv


def gelu_tanh(pre):
    th = jnp.tanh(GELU_A * (pre + GELU_B * (pre * pre * pre)))
    return 0.5 * pre * (1.0 + th), th


def mm(a, b, dims=((1,), (0,))):
    return lax.dot_general(a, b, (dims, ((), ())), preferred_element_type=F32)


def cost(flops, bytes_accessed):
    return pl.CostEstimate(flops=flops, bytes_accessed=bytes_accessed, transcendentals=0)


def fwd_body(n_chunk, x0_ref, w1_ref, w2_ref, xs_ref, pre_ref, y_ref, x_s, n_s, acc_s):
    layer, step = pl.program_id(0), pl.program_id(1)

    @pl.when((layer == 0) & (step == 0))
    def _():
        x_s[...] = x0_ref[...]

    @pl.when(step == 0)
    def _():
        x_f32 = x_s[...].astype(F32)
        n_s[...] = norm_parts(x_f32)[0].astype(BF16)
        acc_s[...] = x_f32
        xs_ref[0] = x_s[...]

    pre = mm(n_s[...], w1_ref[0].astype(BF16))
    pre_ref[0] = pre
    hidden = gelu_tanh(pre)[0].astype(BF16)
    acc_s[...] += mm(hidden, w2_ref[0].astype(BF16))

    @pl.when(step == n_chunk - 1)
    def _():
        out = acc_s[...].astype(BF16)
        x_s[...] = out
        y_ref[...] = out


def forward(x0, w_in, w_out):
    layers, d, ff = w_in.shape
    rows = x0.shape[0]
    n_chunk = ff // CHUNK
    return pl.pallas_call(
        functools.partial(fwd_body, n_chunk),
        grid=(layers, n_chunk),
        in_specs=[
            pl.BlockSpec((rows, d), lambda l, j: (0, 0)),
            pl.BlockSpec((1, d, CHUNK), lambda l, j: (l, 0, j)),
            pl.BlockSpec((1, CHUNK, d), lambda l, j: (l, j, 0)),
        ],
        out_specs=[
            pl.BlockSpec((1, rows, d), lambda l, j: (l, 0, 0)),
            pl.BlockSpec((1, rows, CHUNK), lambda l, j: (l, 0, j)),
            pl.BlockSpec((rows, d), lambda l, j: (0, 0)),
        ],
        out_shape=[
            jax.ShapeDtypeStruct((layers, rows, d), BF16),
            jax.ShapeDtypeStruct((layers, rows, ff), F32),
            jax.ShapeDtypeStruct((rows, d), BF16),
        ],
        scratch_shapes=[pltpu.VMEM((rows, d), BF16), pltpu.VMEM((rows, d), BF16), pltpu.VMEM((rows, d), F32)],
        cost_estimate=cost(4 * layers * rows * d * ff, 8 * layers * d * ff + 4 * layers * rows * ff),
        compiler_params=pltpu.CompilerParams(vmem_limit_bytes=48 << 20),
        name="mlp_forward",
    )(x0, w_in, w_out)


def bwd_body(n_chunk, dtop_ref, xs_ref, pre_ref, w1_ref, w2_ref, g1_ref, g2_ref, dx_ref, d_s, db_s, n_s, dn_s):
    layer, step = pl.program_id(0), pl.program_id(1)

    @pl.when((layer == 0) & (step == 0))
    def _():
        d_s[...] = dtop_ref[...]

    @pl.when(step == 0)
    def _():
        db_s[...] = d_s[...].astype(BF16)
        n_s[...] = norm_parts(xs_ref[0].astype(F32))[0].astype(BF16)
        dn_s[...] = jnp.zeros_like(dn_s)

    pre = pre_ref[0]
    half_out, th = gelu_tanh(pre)
    hidden = half_out.astype(BF16)
    slope = 0.5 * (1.0 + th) + (0.5 * GELU_A) * pre * (1.0 - th * th) * (1.0 + (3.0 * GELU_B) * (pre * pre))
    d_b = db_s[...]
    d_hidden = mm(d_b, w2_ref[0].astype(BF16), ((1,), (1,)))
    d_pre = (slope * d_hidden).astype(BF16)
    g_two = mm(hidden, d_b, ((0,), (0,))).astype(BF16)
    g_one = mm(n_s[...], d_pre, ((0,), (0,))).astype(BF16)
    for part in range(2):
        g1_ref[0, part] = g_one[:, part * LANES:(part + 1) * LANES]
        g2_ref[0, part, 0] = g_two[:, part * LANES:(part + 1) * LANES]
    dn_s[...] += mm(d_pre, w1_ref[0].astype(BF16), ((1,), (1,)))

    @pl.when(step == n_chunk - 1)
    def _():
        normed, inv = norm_parts(xs_ref[0].astype(F32))
        dn = dn_s[...]
        along = jnp.mean(dn * normed, axis=-1, keepdims=True)
        out = d_s[...] + inv * (dn - jnp.mean(dn, axis=-1, keepdims=True) - normed * along)
        d_s[...] = out
        dx_ref[...] = out


def backward(d_top, xs, pre, w_in, w_out, first, count):
    _, d, ff = w_in.shape
    rows = d_top.shape[0]
    n_chunk = ff // CHUNK
    return pl.pallas_call(
        functools.partial(bwd_body, n_chunk),
        grid=(count, n_chunk),
        in_specs=[
            pl.BlockSpec((rows, d), lambda l, j: (0, 0)),
            pl.BlockSpec((1, rows, d), lambda l, j: (first - l, 0, 0)),
            pl.BlockSpec((1, rows, CHUNK), lambda l, j: (first - l, 0, j)),
            pl.BlockSpec((1, d, CHUNK), lambda l, j: (first - l, 0, j)),
            pl.BlockSpec((1, CHUNK, d), lambda l, j: (first - l, j, 0)),
        ],
        out_specs=[
            pl.BlockSpec((1, 2, d, LANES), lambda l, j: (first - l, j, 0, 0)),
            pl.BlockSpec((1, 2, 1, CHUNK, LANES), lambda l, j: (first - l, 0, j, 0, 0)),
            pl.BlockSpec((rows, d), lambda l, j: (0, 0)),
        ],
        out_shape=[
            jax.ShapeDtypeStruct((count, 2 * n_chunk, d, LANES), BF16),
            jax.ShapeDtypeStruct((count, 2, n_chunk, CHUNK, LANES), BF16),
            jax.ShapeDtypeStruct((rows, d), F32),
        ],
        scratch_shapes=[
            pltpu.VMEM((rows, d), F32),
            pltpu.VMEM((rows, d), BF16),
            pltpu.VMEM((rows, d), BF16),
            pltpu.VMEM((rows, d), F32),
        ],
        cost_estimate=cost(8 * count * rows * d * ff, count * (12 * d * ff + 4 * rows * ff)),
        compiler_params=pltpu.CompilerParams(vmem_limit_bytes=56 << 20),
        name="mlp_backward",
    )(d_top, xs, pre, w_in, w_out)


def next_body(n_chunk, n_prev, coef_ref, x0_ref, w1_ref, m1_ref, g1_ref, w2_ref, m2_ref, g2_ref, *rest):
    rest = rest[n_prev:]
    nw1_ref, nm1_ref, nw2_ref, nm2_ref, y_ref, x_s, n_s, acc_s = rest
    layer, step = pl.program_id(0), pl.program_id(1)
    rate, momentum = coef_ref[0], coef_ref[1]

    @pl.when((layer == 0) & (step == 0))
    def _():
        x_s[...] = x0_ref[...]

    @pl.when(step == 0)
    def _():
        x_f32 = x_s[...].astype(F32)
        n_s[...] = norm_parts(x_f32)[0].astype(BF16)
        acc_s[...] = x_f32

    g_one = jnp.concatenate([g1_ref[0, 0], g1_ref[0, 1]], axis=1)
    g_two = jnp.concatenate([g2_ref[0, 0, 0], g2_ref[0, 1, 0]], axis=1)
    m1 = momentum * m1_ref[0] + g_one.astype(F32)
    w1 = w1_ref[0] - rate * m1
    nm1_ref[0] = m1
    nw1_ref[0] = w1
    m2 = momentum * m2_ref[0] + g_two.astype(F32)
    w2 = w2_ref[0] - rate * m2
    nm2_ref[0] = m2
    nw2_ref[0] = w2
    pre = mm(n_s[...], w1.astype(BF16))
    hidden = gelu_tanh(pre)[0].astype(BF16)
    acc_s[...] += mm(hidden, w2.astype(BF16))

    @pl.when(step == n_chunk - 1)
    def _():
        out = acc_s[...].astype(BF16)
        x_s[...] = out
        y_ref[...] = out


def update_forward(coef, x0, w_in, mom_in, g_in, w_out, mom_out, g_out, first, count, prev):
    layers, d, ff = w_in.shape
    rows = x0.shape[0]
    n_chunk = ff // CHUNK
    in_block = pl.BlockSpec((1, d, CHUNK), lambda l, j: (first + l, 0, j))
    out_block = pl.BlockSpec((1, CHUNK, d), lambda l, j: (first + l, j, 0))
    n_prev = 0 if prev is None else 4
    return pl.pallas_call(
        functools.partial(next_body, n_chunk, n_prev),
        grid=(count, n_chunk),
        in_specs=[
            pl.BlockSpec(memory_space=pltpu.SMEM),
            pl.BlockSpec((rows, d), lambda l, j: (0, 0)),
            in_block,
            in_block,
            pl.BlockSpec((1, 2, d, LANES), lambda l, j: (l, j, 0, 0)),
            out_block,
            out_block,
            pl.BlockSpec((1, 2, 1, CHUNK, LANES), lambda l, j: (l, 0, j, 0, 0)),
        ] + [pl.BlockSpec(memory_space=pl.ANY)] * n_prev,
        out_specs=[in_block, in_block, out_block, out_block, pl.BlockSpec((rows, d), lambda l, j: (0, 0))],
        out_shape=[
            jax.ShapeDtypeStruct(w_in.shape, F32),
            jax.ShapeDtypeStruct(w_in.shape, F32),
            jax.ShapeDtypeStruct(w_out.shape, F32),
            jax.ShapeDtypeStruct(w_out.shape, F32),
            jax.ShapeDtypeStruct((rows, d), BF16),
        ],
        scratch_shapes=[pltpu.VMEM((rows, d), BF16), pltpu.VMEM((rows, d), BF16), pltpu.VMEM((rows, d), F32)],
        input_output_aliases={8 + i: i for i in range(n_prev)},
        cost_estimate=cost(4 * count * rows * d * ff, 36 * count * d * ff),
        compiler_params=pltpu.CompilerParams(vmem_limit_bytes=48 << 20),
        name="update_forward",
    )(coef, x0, w_in, mom_in, g_in, w_out, mom_out, g_out, *(prev or ()))


def sum_body(n, layers, g1_ref, g2_ref, o1_ref, o2_ref, work, land0, land1, land2, land3,
             load_sem, d0_send, d0_recv, ring_send, ring_recv, d1_send, d1_recv, out_sem):
    rows = work.shape[2]
    sub = (rows, rows // n, rows // (n * n))
    me = lax.axis_index('data')
    core = lax.rem(me, 2)
    partner = me + 1 - 2 * core
    own, other = core * n, (1 - core) * n
    strides = (2, 2 * n, 2 * n * n)
    pos = [lax.rem(lax.div(me, stride), n) for stride in strides]
    last = n - 1
    messages = 6 * last

    def neighbour(axis, way):
        return me + (lax.rem(pos[axis] + way + n, n) - pos[axis]) * strides[axis]

    barrier = pltpu.get_barrier_semaphore()
    greeted = [partner] + [neighbour(axis, way) for axis in range(3) for way in (1, -1)]
    for device in greeted:
        pl.semaphore_signal(barrier, inc=1, device_id=(device,), device_id_type=MESH_ID)
    pl.semaphore_wait(barrier, len(greeted))

    def each(fn):
        @pl.loop(0, layers // 3)
        def _(i):
            for colour in range(3):
                for kind in range(2):
                    way = 1 - 2 * lax.rem(i, 2)
                    way = way if kind == 0 else -way
                    layer = colour + 3 * i
                    fn((g1_ref, g2_ref)[kind], (o1_ref, o2_ref)[kind], kind * layers + layer, layer, colour, way)

    def at(base, way, steps):
        return lax.rem(base - way * steps + 2 * n, n)

    def remote(src, dst, send, recv, device):
        return pltpu.make_async_remote_copy(src_ref=src, dst_ref=dst, send_sem=send, recv_sem=recv, device_id=(device,), device_id_type=MESH_ID)

    def load_copy(g_ref, m, layer, block, k):
        return pltpu.make_async_copy(g_ref.at[layer, own + block], work.at[m, own + block], load_sem.at[m, k])

    def swap_copy(g_ref, m, layer, block, k):
        return remote(g_ref.at[layer, other + block], land0.at[m, block], d0_send.at[m, k], d0_recv.at[m, k], partner)

    def share_copy(m, block, k, half):
        return remote(work.at[m, half + block], work.at[m, half + block], d1_send.at[m], d1_recv.at[m, k], partner)

    def place(m, colour, way, stage):
        block = at(pos[colour], way, last)
        row = 0
        if stage == 3:
            row = at(pos[(colour + 1) % 3], way, last) * sub[1]
        return block, row

    def piece(m, colour, way, stage, index):
        if stage == 1:
            return work.at[m, own + index]
        block, row = place(m, colour, way, stage)
        return work.at[m, own + block, pl.ds(pl.multiple_of(row + index * sub[stage - 1], sub[stage - 1]), sub[stage - 1])]

    lands = (None, land1, land2, land3)

    def message(t, m, colour, way):
        phase, s = divmod(t, last)
        stage = (1, 2, 3, 3, 2, 1)[phase]
        axis = (colour + stage - 1) % 3
        to = neighbour(axis, way)
        if phase < 3:
            src = piece(m, colour, way, stage, at(pos[axis], way, s))
            dst = lands[stage].at[m, s]
        else:
            src = piece(m, colour, way, stage, at(pos[axis], way, last + s))
            dst = src
        return remote(src, dst, ring_send.at[m], ring_recv.at[m, t], to)

    def arrival(t, m, colour, way):
        phase, s = divmod(t, last)
        stage = (1, 2, 3, 3, 2, 1)[phase]
        axis = (colour + stage - 1) % 3
        if phase < 3:
            dst = lands[stage].at[m, s]
        else:
            dst = piece(m, colour, way, stage, at(pos[axis], way, last + s + 1))
        return remote(dst, dst, ring_send.at[m], ring_recv.at[m, t], neighbour(axis, way))

    def accumulate(dst, sources):
        count = dst.shape[0]
        step = min(count, 64)

        @pl.loop(0, count // step)
        def _(r):
            part = pl.ds(pl.multiple_of(r * step, step), step)
            total = dst[part, :].astype(F32)
            for source in sources:
                total = total + source[part, :].astype(F32)
            dst[part, :] = total.astype(BF16)

    for k in range(n):
        def begin(g_ref, o_ref, m, layer, colour, way, k=k):
            block = at(pos[colour], way, k)
            swap_copy(g_ref, m, layer, block, k).start()
            load_copy(g_ref, m, layer, block, k).start()
        each(begin)

    for t in range(messages + 1):
        def tick(g_ref, o_ref, m, layer, colour, way, t=t):
            if t > 0:
                arrival(t - 1, m, colour, way).wait_recv()
                message(t - 1, m, colour, way).wait_send()
            if t <= last:
                block = at(pos[colour], way, t)
                load_copy(g_ref, m, layer, block, t).wait()
                swap_copy(g_ref, m, layer, block, t).wait_recv()
                sources = [land0.at[m, block]] + ([land1.at[m, t - 1]] if t > 0 else [])
                accumulate(work.at[m, own + block], sources)
            elif t <= 3 * last:
                phase, s = divmod(t - 1, last)
                axis = (colour + phase) % 3
                accumulate(piece(m, colour, way, phase + 1, at(pos[axis], way, s + 1)), [lands[phase + 1].at[m, s]])
            if t < messages:
                message(t, m, colour, way).start()
            k = t - 5 * last
            if k >= 0:
                if k > 0:
                    share_copy(m, at(pos[colour], way, last + k - 1), k - 1, own).wait_send()
                share_copy(m, at(pos[colour], way, last + k), k, own).start()
        each(tick)

    def finish(g_ref, o_ref, m, layer, colour, way):
        share_copy(m, at(pos[colour], way, last + last), last, own).wait_send()
        for k in range(n):
            share_copy(m, at(pos[colour], way, last + k), k, other).wait_recv()
            swap_copy(g_ref, m, layer, at(pos[colour], way, k), k).wait_send()
        pltpu.make_async_copy(work.at[m], o_ref.at[layer], out_sem.at[m]).start()
    each(finish)

    def drain(g_ref, o_ref, m, layer, colour, way):
        pltpu.make_async_copy(work.at[m], o_ref.at[layer], out_sem.at[m]).wait()
    each(drain)


def sum_gradients(g1, g2, group_size):
    n = round((group_size // 2) ** (1 / 3))
    layers, blocks, rows, lanes = g1.shape
    count = 2 * layers
    dma = pltpu.SemaphoreType.DMA
    messages = 6 * (n - 1)
    return pl.pallas_call(
        functools.partial(sum_body, n, layers),
        in_specs=[pl.BlockSpec(memory_space=pl.ANY)] * 2,
        out_specs=[pl.BlockSpec(memory_space=pl.ANY)] * 2,
        out_shape=[jax.ShapeDtypeStruct(g1.shape, BF16), jax.ShapeDtypeStruct(g2.shape, BF16)],
        scratch_shapes=[
            pltpu.VMEM((count, blocks, rows, lanes), BF16),
            pltpu.VMEM((count, n, rows, lanes), BF16),
            pltpu.VMEM((count, n - 1, rows, lanes), BF16),
            pltpu.VMEM((count, n - 1, rows // n, lanes), BF16),
            pltpu.VMEM((count, n - 1, rows // (n * n), lanes), BF16),
            dma((count, n)),
            dma((count, n)),
            dma((count, n)),
            dma((count,)),
            dma((count, messages)),
            dma((count,)),
            dma((count, n)),
            dma((count,)),
        ],
        cost_estimate=cost(1 << 30, 4 * g1.size),
        compiler_params=pltpu.CompilerParams(collective_id=0, has_side_effects=True, vmem_limit_bytes=58 << 20),
        name="gradient_sum",
    )(g1, g2)


def pool(tok_act, images):
    return jnp.mean(tok_act.reshape(images, -1, tok_act.shape[-1]), axis=1, dtype=F32).astype(BF16)


def head_backward(tok_act, lab_row, w_head_b, examples):
    images = lab_row.shape[0]
    seq = tok_act.shape[0] // images
    pooled = pool(tok_act, images)
    logits = jnp.dot(pooled, w_head_b, preferred_element_type=F32)
    soft_prob = jax.nn.softmax(logits, axis=-1)
    onehot = (lab_row[:, None] == jnp.arange(logits.shape[1])[None, :]).astype(F32)
    d_logits = ((soft_prob - onehot) / examples).astype(BF16)
    g_head = jnp.einsum('bd,bc->dc', pooled, d_logits, preferred_element_type=F32)
    d_pooled = jnp.einsum('bc,dc->bd', d_logits, w_head_b, preferred_element_type=F32)
    d_top = jnp.broadcast_to((d_pooled / seq)[:, None, :], (images, seq, tok_act.shape[1]))
    return g_head, d_top.reshape(tok_act.shape)


def solution(mesh):
    group_size = mesh.shape['data']

    def local_step(x_step, labels, x_next, w_in, w_out, w_head, mom_in, mom_out, mom_head, learn_rate, mom_coef):
        micro_count, images, seq, d = x_step.shape
        layers = w_in.shape[0]
        examples = micro_count * images * group_size
        xs, pre, top = forward(x_step.reshape(-1, d), w_in, w_out)
        w_head_b = w_head.astype(BF16)
        g_head, d_act = head_backward(top, labels.reshape(-1), w_head_b, examples)
        red_head = lax.psum(g_head.astype(BF16), 'data')
        g_in, g_out, _ = backward(d_act, xs, pre, w_in, w_out, layers - 1, layers)
        block_shape = (layers, -1) + g_out.shape[3:]
        red_in, red_out = sum_gradients(g_in, g_out.reshape(block_shape), group_size)
        coef = jnp.stack([learn_rate, mom_coef])
        tok = x_next.reshape(-1, d)
        new_w_in, new_mom_in, new_w_out, new_mom_out, tok = update_forward(coef, tok, w_in, mom_in, red_in, w_out, mom_out, red_out.reshape(g_out.shape), 0, layers, None)
        new_mom_head = mom_coef * mom_head + red_head.astype(F32)
        new_w_head = w_head - learn_rate * new_mom_head
        logits_next = jnp.dot(pool(tok, images), new_w_head.astype(BF16), preferred_element_type=F32)
        return (logits_next, new_w_in, new_w_out, new_w_head, new_mom_in, new_mom_out, new_mom_head)

    return jax.shard_map(local_step, mesh=mesh, in_specs=(P(None, 'data', None, None), P(None, 'data'), P('data', None, None), P(), P(), P(), P(), P(), P(), P(), P()), out_specs=(P('data', None), P(), P(), P(), P(), P(), P()), check_vma=False)
```

```python
import functools

import jax
import jax.numpy as jnp
from jax import lax
from jax.experimental import pallas as pl
from jax.experimental.pallas import tpu as pltpu
from jax.sharding import PartitionSpec as P

LN_EPS = 1e-6
GELU_A = 0.7978845608028654
GELU_B = 0.044715
CHUNK = 512
UPD_CHUNK = 1024
FWD_CHUNK = 1024
RING = 4
LANES = 256
MESH_ID = pl.DeviceIdType.MESH
F32 = jnp.float32
BF16 = jnp.bfloat16


def norm_parts(x_f32):
    row_mean = jnp.mean(x_f32, axis=-1, keepdims=True)
    centered = x_f32 - row_mean
    row_var = jnp.mean(centered * centered, axis=-1, keepdims=True)
    inv = lax.rsqrt(row_var + LN_EPS)
    return centered * inv, inv


def gelu_tanh(pre):
    square = pre * pre
    half = 0.5 + 0.5 * jnp.tanh(pre * (GELU_A + (GELU_A * GELU_B) * square))
    return pre * half, half, square


def mm(a, b, dims=((1,), (0,))):
    return lax.dot_general(a, b, (dims, ((), ())), preferred_element_type=F32)


def image_sums(tok_act, images):
    rows = tok_act.shape[0]
    seq = rows // images
    start = lax.broadcasted_iota(jnp.int32, (16, rows), 0) * seq
    row = lax.broadcasted_iota(jnp.int32, (16, rows), 1)
    pick = ((row >= start) & (row < start + seq)).astype(F32).astype(BF16)
    return mm(pick, tok_act)


def cost(flops, bytes_accessed):
    return pl.CostEstimate(flops=flops, bytes_accessed=bytes_accessed, transcendentals=0)


def fwd_body(n_chunk, images, x0_ref, w1_ref, w2_ref, xs_ref, pre_ref, y_ref, x_s, n_s, acc_s):
    layer, step = pl.program_id(0), pl.program_id(1)

    @pl.when((layer == 0) & (step == 0))
    def _():
        x_s[...] = x0_ref[...]

    @pl.when(step == 0)
    def _():
        x_f32 = x_s[...].astype(F32)
        n_s[...] = norm_parts(x_f32)[0].astype(BF16)
        acc_s[...] = x_f32
        xs_ref[0] = x_s[...]

    pre = mm(n_s[...], w1_ref[0].astype(BF16))
    pre_ref[0] = pre
    hidden = gelu_tanh(pre)[0].astype(BF16)
    acc_s[...] += mm(hidden, w2_ref[0].astype(BF16))

    @pl.when(step == n_chunk - 1)
    def _():
        out = acc_s[...].astype(BF16)
        x_s[...] = out
        y_ref[...] = image_sums(out, images)


def forward(x0, images, w_in, w_out):
    layers, d, ff = w_in.shape
    rows = x0.shape[0]
    n_chunk = ff // FWD_CHUNK
    return pl.pallas_call(
        functools.partial(fwd_body, n_chunk, images),
        grid=(layers, n_chunk),
        in_specs=[
            pl.BlockSpec((rows, d), lambda l, j: (0, 0)),
            pl.BlockSpec((1, d, FWD_CHUNK), lambda l, j: (l, 0, j)),
            pl.BlockSpec((1, FWD_CHUNK, d), lambda l, j: (l, j, 0)),
        ],
        out_specs=[
            pl.BlockSpec((1, rows, d), lambda l, j: (l, 0, 0)),
            pl.BlockSpec((1, rows, FWD_CHUNK), lambda l, j: (l, 0, j)),
            pl.BlockSpec((16, d), lambda l, j: (0, 0)),
        ],
        out_shape=[
            jax.ShapeDtypeStruct((layers, rows, d), BF16),
            jax.ShapeDtypeStruct((layers, rows, ff), F32),
            jax.ShapeDtypeStruct((16, d), F32),
        ],
        scratch_shapes=[pltpu.VMEM((rows, d), BF16), pltpu.VMEM((rows, d), BF16), pltpu.VMEM((rows, d), F32)],
        cost_estimate=cost(4 * layers * rows * d * ff, 8 * layers * d * ff + 4 * layers * rows * ff),
        compiler_params=pltpu.CompilerParams(vmem_limit_bytes=48 << 20),
        name="mlp_forward",
    )(x0, w_in, w_out)


def bwd_body(n_chunk, images, dtop_ref, xs_ref, pre_ref, w1_ref, w2_ref, g1_ref, g2_ref, d_s, db_s, n_s, dn_s):
    layer, step = pl.program_id(0), pl.program_id(1)

    @pl.when((layer == 0) & (step == 0))
    def _():
        rows = d_s.shape[0]
        row = lax.broadcasted_iota(jnp.int32, d_s.shape, 0)
        value = jnp.broadcast_to(dtop_ref[0:1, :], d_s.shape)
        for image in range(1, images):
            value = jnp.where(row >= image * (rows // images), dtop_ref[image:image + 1, :], value)
        d_s[...] = value

    @pl.when(step == 0)
    def _():
        db_s[...] = d_s[...].astype(BF16)
        n_s[...] = norm_parts(xs_ref[0].astype(F32))[0].astype(BF16)
        dn_s[...] = jnp.zeros_like(dn_s)

    pre = pre_ref[0]
    gelu, half, square = gelu_tanh(pre)
    hidden = gelu.astype(BF16)
    slope = half + (pre * half) * ((1.0 - half) * (2.0 * GELU_A + (6.0 * GELU_A * GELU_B) * square))
    d_b = db_s[...]
    d_hidden = mm(d_b, w2_ref[0].astype(BF16), ((1,), (1,)))
    d_pre = (slope * d_hidden).astype(BF16)
    g_two = mm(hidden, d_b, ((0,), (0,))).astype(BF16)
    g_one = mm(n_s[...], d_pre, ((0,), (0,))).astype(BF16)
    for part in range(2):
        g1_ref[0, part] = g_one[:, part * LANES:(part + 1) * LANES]
        g2_ref[0, part, 0] = g_two[:, part * LANES:(part + 1) * LANES]
    dn_s[...] += mm(d_pre, w1_ref[0].astype(BF16), ((1,), (1,)))

    @pl.when(step == n_chunk - 1)
    def _():
        normed, inv = norm_parts(xs_ref[0].astype(F32))
        dn = dn_s[...]
        along = jnp.mean(dn * normed, axis=-1, keepdims=True)
        out = d_s[...] + inv * (dn - jnp.mean(dn, axis=-1, keepdims=True) - normed * along)
        d_s[...] = out


def backward(d_top, images, xs, pre, w_in, w_out, first, count):
    _, d, ff = w_in.shape
    rows = xs.shape[1]
    n_chunk = ff // CHUNK
    return pl.pallas_call(
        functools.partial(bwd_body, n_chunk, images),
        grid=(count, n_chunk),
        in_specs=[
            pl.BlockSpec(d_top.shape, lambda l, j: (0, 0)),
            pl.BlockSpec((1, rows, d), lambda l, j: (first - l, 0, 0)),
            pl.BlockSpec((1, rows, CHUNK), lambda l, j: (first - l, 0, j)),
            pl.BlockSpec((1, d, CHUNK), lambda l, j: (first - l, 0, j)),
            pl.BlockSpec((1, CHUNK, d), lambda l, j: (first - l, j, 0)),
        ],
        out_specs=[
            pl.BlockSpec((1, 2, d, LANES), lambda l, j: (first - l, j, 0, 0)),
            pl.BlockSpec((1, 2, 1, CHUNK, LANES), lambda l, j: (first - l, 0, j, 0, 0)),
        ],
        out_shape=[
            jax.ShapeDtypeStruct((count, 2 * n_chunk, d, LANES), BF16),
            jax.ShapeDtypeStruct((count, 2, n_chunk, CHUNK, LANES), BF16),
        ],
        scratch_shapes=[
            pltpu.VMEM((rows, d), F32),
            pltpu.VMEM((rows, d), BF16),
            pltpu.VMEM((rows, d), BF16),
            pltpu.VMEM((rows, d), F32),
        ],
        cost_estimate=cost(8 * count * rows * d * ff, count * (12 * d * ff + 4 * rows * ff)),
        compiler_params=pltpu.CompilerParams(vmem_limit_bytes=56 << 20),
        name="mlp_backward",
    )(d_top, xs, pre, w_in, w_out)


def next_body(n_chunk, images, coef_ref, x0_ref, w1_ref, m1_ref, g1_ref, w2_ref, m2_ref, g2_ref,
              nw1_ref, nm1_ref, nw2_ref, nm2_ref, y_ref, x_s, n_s, acc_s):
    layer, step = pl.program_id(0), pl.program_id(1)
    rate, momentum = coef_ref[0], coef_ref[1]

    @pl.when((layer == 0) & (step == 0))
    def _():
        x_s[...] = x0_ref[...]

    @pl.when(step == 0)
    def _():
        x_f32 = x_s[...].astype(F32)
        n_s[...] = norm_parts(x_f32)[0].astype(BF16)
        acc_s[...] = x_f32

    g_one = jnp.concatenate([g1_ref[0, 0], g1_ref[0, 1], g1_ref[0, 2], g1_ref[0, 3]], axis=1)
    g_two = jnp.concatenate([jnp.concatenate([g2_ref[0, 0, r], g2_ref[0, 1, r]], axis=1) for r in range(2)], axis=0)
    m1 = momentum * m1_ref[0] + g_one.astype(F32)
    w1 = w1_ref[0] - rate * m1
    nm1_ref[0] = m1
    nw1_ref[0] = w1
    m2 = momentum * m2_ref[0] + g_two.astype(F32)
    w2 = w2_ref[0] - rate * m2
    nm2_ref[0] = m2
    nw2_ref[0] = w2
    pre = mm(n_s[...], w1.astype(BF16))
    hidden = gelu_tanh(pre)[0].astype(BF16)
    acc_s[...] += mm(hidden, w2.astype(BF16))

    @pl.when(step == n_chunk - 1)
    def _():
        out = acc_s[...].astype(BF16)
        x_s[...] = out
        y_ref[...] = image_sums(out, images)


def update_forward(coef, x0, images, w_in, mom_in, g_in, w_out, mom_out, g_out):
    layers, d, ff = w_in.shape
    rows = x0.shape[0]
    n_chunk = ff // UPD_CHUNK
    in_block = pl.BlockSpec((1, d, UPD_CHUNK), lambda l, j: (l, 0, j))
    out_block = pl.BlockSpec((1, UPD_CHUNK, d), lambda l, j: (l, j, 0))
    return pl.pallas_call(
        functools.partial(next_body, n_chunk, images),
        grid=(layers, n_chunk),
        in_specs=[
            pl.BlockSpec(memory_space=pltpu.SMEM),
            pl.BlockSpec((rows, d), lambda l, j: (0, 0)),
            in_block,
            in_block,
            pl.BlockSpec((1, 4, d, LANES), lambda l, j: (l, j, 0, 0)),
            out_block,
            out_block,
            pl.BlockSpec((1, 2, 2, 512, LANES), lambda l, j: (l, 0, j, 0, 0)),
        ],
        out_specs=[in_block, in_block, out_block, out_block, pl.BlockSpec((16, d), lambda l, j: (0, 0))],
        out_shape=[
            jax.ShapeDtypeStruct(w_in.shape, F32),
            jax.ShapeDtypeStruct(w_in.shape, F32),
            jax.ShapeDtypeStruct(w_out.shape, F32),
            jax.ShapeDtypeStruct(w_out.shape, F32),
            jax.ShapeDtypeStruct((16, d), F32),
        ],
        scratch_shapes=[pltpu.VMEM((rows, d), BF16), pltpu.VMEM((rows, d), BF16), pltpu.VMEM((rows, d), F32)],
        cost_estimate=cost(4 * layers * rows * d * ff, 36 * layers * d * ff),
        compiler_params=pltpu.CompilerParams(vmem_limit_bytes=60 << 20),
        name="update_forward",
    )(coef, x0, w_in, mom_in, g_in, w_out, mom_out, g_out)


def sum_body(layers, g1_ref, g2_ref, head_ref, o1_ref, o2_ref, all_ref, work, land0, land1, land2, land3, turn, head,
             load_sem, d0_send, d0_recv, ring_send, ring_recv, d1_send, d1_recv, out_sem, head_send, head_recv, head_sem):
    n = RING
    rows = work.shape[2]
    sub = (rows, rows // n, rows // (n * n))
    me = lax.axis_index('data')
    core = lax.rem(me, 2)
    partner = me + 1 - 2 * core
    own, other = core * n, (1 - core) * n
    strides = (2, 2 * n, 2 * n * n)
    pos = [lax.rem(lax.div(me, stride), n) for stride in strides]
    near = [me + (1 - 2 * lax.rem(p, 2)) * stride for p, stride in zip(pos, strides)]
    far = [me + (3 - 2 * p) * stride for p, stride in zip(pos, strides)]
    near_bit = [lax.rem(lax.div(p + 1, 2), 2) for p in pos]
    far_bit = [lax.div(p, 2) for p in pos]

    barrier = pltpu.get_barrier_semaphore()
    greeted = [partner] + near + far
    for device in greeted:
        pl.semaphore_signal(barrier, inc=1, device_id=(device,), device_id_type=MESH_ID)
    pl.semaphore_wait(barrier, len(greeted))

    def each(fn):
        @pl.loop(0, layers // 3)
        def _(i):
            for colour in range(3):
                for kind in range(2):
                    flip = lax.rem(i + kind, 2)
                    layer = colour + 3 * i
                    fn((g1_ref, g2_ref)[kind], (o1_ref, o2_ref)[kind], kind * layers + layer, layer, colour, flip)

    def remote(src, dst, send, recv, device):
        return pltpu.make_async_remote_copy(src_ref=src, dst_ref=dst, send_sem=send, recv_sem=recv, device_id=(device,), device_id_type=MESH_ID)

    def mix(a, b, flip):
        return a + flip * (b - a)

    def bits(colour, flip, stage):
        axis = (colour + stage - 1) % 3
        return mix(near_bit[axis], far_bit[axis], flip), mix(far_bit[axis], near_bit[axis], flip)

    def unit(colour, flip, stage):
        hi, lo = bits(colour, flip, stage)
        return 2 * hi + lo

    def units(m, colour, flip, stage, first, count):
        if stage == 1:
            return work.at[m, pl.ds(own + first, count)]
        row = first * sub[stage - 1]
        if stage == 3:
            row = row + unit(colour, flip, 2) * sub[1]
        row = pl.multiple_of(row, sub[stage - 1])
        return work.at[m, pl.ds(own + unit(colour, flip, 1), 1), pl.ds(row, count * sub[stage - 1])]

    def land(m, stage, step):
        first, count = ((0, 2), (2, 1))[step]
        if stage == 1:
            return land1.at[m, pl.ds(first, count)]
        size = sub[stage - 1]
        return (land2, land3)[stage - 2].at[pl.ds(m, 1), pl.ds(first * size, count * size)]

    def land_unit(m, which):
        return land3.at[pl.ds(m, 1), pl.ds(pl.multiple_of(which * sub[2], sub[2]), sub[2])]

    def copies(t, m, colour, flip):
        scatter = t < 6
        stage = t // 2 + 1 if scatter else 6 - t // 2
        step = t % 2
        hi, lo = bits(colour, flip, stage)
        axis = (colour + stage - 1) % 3
        with_first = (step == 0) == scatter
        to = mix(near[axis], far[axis], flip) if with_first else mix(far[axis], near[axis], flip)
        kept = (2 * hi, 2) if with_first else (2 * hi + lo, 1)
        given = (2 - 2 * hi, 2) if with_first else (2 * hi + 1 - lo, 1)
        if scatter:
            src = turn.at[pl.ds(m, 1)] if t == 5 else units(m, colour, flip, stage, *given)
            return src, land(m, stage, step), land(m, stage, step), to, kept
        src = units(m, colour, flip, stage, *kept)
        return src, src, units(m, colour, flip, stage, *given), to, given

    def message(t, m, colour, flip):
        src, dst, _, to, _ = copies(t, m, colour, flip)
        return remote(src, dst, ring_send.at[m], ring_recv.at[m, t], to)

    def arrival(t, m, colour, flip):
        _, _, here, to, _ = copies(t, m, colour, flip)
        return remote(here, here, ring_send.at[m], ring_recv.at[m, t], to)

    def pair(colour, flip, k):
        hi, _ = bits(colour, flip, 1)
        return mix(2 - 2 * hi, 2 * hi, k)

    def load_copy(g_ref, m, layer, colour, flip, k):
        blocks = pl.ds(own + pair(colour, flip, k), 2)
        return pltpu.make_async_copy(g_ref.at[layer, blocks], work.at[m, blocks], load_sem.at[m, k])

    def swap_copy(g_ref, m, layer, colour, flip, k):
        first = pair(colour, flip, k)
        return remote(g_ref.at[layer, pl.ds(other + first, 2)], land0.at[m, pl.ds(first, 2)], d0_send.at[m, k], d0_recv.at[m, k], partner)

    def final(colour, flip, k):
        hi, lo = bits(colour, flip, 1)
        return ((2 * hi + lo, 1), (2 * hi + 1 - lo, 1), (2 - 2 * hi, 2))[k]

    def share_copy(m, colour, flip, k, half):
        first, count = final(colour, flip, k)
        blocks = work.at[m, pl.ds(half + first, count)]
        return remote(blocks, blocks, d1_send.at[m, k], d1_recv.at[m, k], partner)

    def out_copy(o_ref, m, layer, colour, flip, k, half, slot):
        first, count = final(colour, flip, k)
        blocks = pl.ds(half + first, count)
        return pltpu.make_async_copy(work.at[m, blocks], o_ref.at[layer, blocks], out_sem.at[m, slot])

    def accumulate(dst, sources):
        blocks, count, _ = dst.shape
        step = min(count, 64)

        @pl.loop(0, count // step)
        def _(r):
            part = pl.ds(pl.multiple_of(r * step, step), step)
            for block in range(blocks):
                total = sources[0][block, part, :].astype(F32)
                for source in sources[1:]:
                    total = total + source[block, part, :].astype(F32)
                dst[block, part, :] = total.astype(BF16)

    head_way = 1 - 2 * core

    def head_message(j, back):
        axis, s = divmod(j, n - 1)
        index = lax.rem(pos[axis] - head_way * (s + back) + 2 * n, n)
        to = me + (lax.rem(pos[axis] + head_way + n, n) - pos[axis]) * strides[axis]
        if axis == 0:
            part = head.at[core, pos[2], pos[1], index]
        elif axis == 1:
            part = head.at[core, pos[2], index]
        else:
            part = head.at[core, index]
        return remote(part, part, head_send, head_recv.at[j], to)

    def head_share(which):
        return remote(head.at[which], head.at[which], head_send, head_recv.at[3 * (n - 1)], partner)

    def head_tick(t):
        count = 3 * (n - 1)
        if t == 0:
            first = pltpu.make_async_copy(head_ref, head.at[core, pos[2], pos[1], pos[0]], head_sem)
            first.start()
            first.wait()
        elif t <= count:
            head_message(t - 1, 1).wait_recv()
            head_message(t - 1, 0).wait_send()
        if t < count:
            head_message(t, 0).start()
        elif t == count:
            head_share(core).start()

    for k in range(2):
        def begin(g_ref, o_ref, m, layer, colour, flip, k=k):
            swap_copy(g_ref, m, layer, colour, flip, k).start()
            load_copy(g_ref, m, layer, colour, flip, k).start()
        each(begin)

    for t in range(13):
        def tick(g_ref, o_ref, m, layer, colour, flip, t=t):
            if t > 0:
                arrival(t - 1, m, colour, flip).wait_recv()
                message(t - 1, m, colour, flip).wait_send()
            if t < 2:
                load_copy(g_ref, m, layer, colour, flip, t).wait()
                swap_copy(g_ref, m, layer, colour, flip, t).wait_recv()
                blocks = units(m, colour, flip, 1, pair(colour, flip, t), 2)
                sources = [land0.at[m, pl.ds(pair(colour, flip, t), 2)]] + ([land(m, 1, 0)] if t > 0 else [])
                accumulate(blocks, [blocks] + sources)
            elif t == 5:
                hi, lo = bits(colour, flip, 3)
                mine, theirs = units(m, colour, flip, 3, 2 * hi + lo, 1), units(m, colour, flip, 3, 2 * hi + 1 - lo, 1)
                accumulate(turn.at[pl.ds(m, 1)], [theirs, land_unit(m, 1 - lo)])
                accumulate(mine, [mine, land_unit(m, lo)])
            elif t < 7:
                _, _, here, _, kept = copies(t - 1, m, colour, flip)
                blocks = units(m, colour, flip, (t + 1) // 2, *kept)
                accumulate(blocks, [blocks, here])
            if t < 12:
                message(t, m, colour, flip).start()
            k = t - 10
            if k >= 0:
                share_copy(m, colour, flip, k, own).start()
                out_copy(o_ref, m, layer, colour, flip, k, own, k).start()
            if k >= 1:
                share_copy(m, colour, flip, k - 1, other).wait_recv()
                out_copy(o_ref, m, layer, colour, flip, k - 1, other, k + 2).start()
        each(tick)
        head_tick(t)

    head_share(1 - core).wait_recv()
    head_share(core).wait_send()
    head_out = pltpu.make_async_copy(head, all_ref, head_sem)
    head_out.start()

    def finish(g_ref, o_ref, m, layer, colour, flip):
        share_copy(m, colour, flip, 2, other).wait_recv()
        out_copy(o_ref, m, layer, colour, flip, 2, other, 5).start()
    each(finish)

    def drain(g_ref, o_ref, m, layer, colour, flip):
        for k in range(3):
            share_copy(m, colour, flip, k, own).wait_send()
            out_copy(o_ref, m, layer, colour, flip, k, own, k).wait()
            out_copy(o_ref, m, layer, colour, flip, k, other, k + 3).wait()
        for k in range(2):
            swap_copy(g_ref, m, layer, colour, flip, k).wait_send()
    each(drain)
    head_out.wait()


def sum_gradients(g1, g2, head_part, group_size):
    n = RING
    if group_size != 2 * n ** 3:
        raise ValueError("needs a 4x4x4 torus")
    layers, blocks, rows, lanes = g1.shape
    count = 2 * layers
    dma = pltpu.SemaphoreType.DMA
    head_shape = (2, n, n, n) + head_part.shape
    return pl.pallas_call(
        functools.partial(sum_body, layers),
        in_specs=[pl.BlockSpec(memory_space=pl.ANY)] * 3,
        out_specs=[pl.BlockSpec(memory_space=pl.ANY)] * 3,
        out_shape=[
            jax.ShapeDtypeStruct(g1.shape, BF16),
            jax.ShapeDtypeStruct(g2.shape, BF16),
            jax.ShapeDtypeStruct(head_shape, BF16),
        ],
        scratch_shapes=[
            pltpu.VMEM((count, blocks, rows, lanes), BF16),
            pltpu.VMEM((count, n, rows, lanes), BF16),
            pltpu.VMEM((count, 3, rows, lanes), BF16),
            pltpu.VMEM((count, 3 * rows // n, lanes), BF16),
            pltpu.VMEM((count, 3 * rows // (n * n), lanes), BF16),
            pltpu.VMEM((count, rows // (n * n), lanes), BF16),
            pltpu.VMEM(head_shape, BF16),
            dma((count, 2)),
            dma((count, 2)),
            dma((count, 2)),
            dma((count,)),
            dma((count, 12)),
            dma((count, 3)),
            dma((count, 3)),
            dma((count, 6)),
            dma,
            dma((3 * (n - 1) + 1,)),
            dma,
        ],
        cost_estimate=cost(1 << 30, 4 * g1.size),
        compiler_params=pltpu.CompilerParams(collective_id=0, has_side_effects=True, vmem_limit_bytes=60 << 20),
        name="gradient_sum",
    )(g1, g2, head_part)


def head_backward(pooled, lab_row, w_head_b, examples):
    logits = jnp.dot(pooled, w_head_b, preferred_element_type=F32)
    soft_prob = jax.nn.softmax(logits, axis=-1)
    onehot = (lab_row[:, None] == jnp.arange(logits.shape[1])[None, :]).astype(F32)
    d_logits = ((soft_prob - onehot) / examples).astype(BF16)
    d_pooled = jnp.einsum('bc,dc->bd', d_logits, w_head_b, preferred_element_type=F32)
    return d_logits, d_pooled


def solution(mesh):
    group_size = mesh.shape['data']

    def local_step(x_step, labels, x_next, w_in, w_out, w_head, mom_in, mom_out, mom_head, learn_rate, mom_coef):
        micro_count, images, seq, d = x_step.shape
        layers = w_in.shape[0]
        classes = w_head.shape[1]
        batch = micro_count * images
        examples = batch * group_size
        xs, pre, sums = forward(x_step.reshape(-1, d), batch, w_in, w_out)
        pooled = (sums[:batch] / seq).astype(BF16)
        d_logits, d_pooled = head_backward(pooled, labels.reshape(-1), w_head.astype(BF16), examples)
        wide = -(-classes // 512) * 512
        head_part = jnp.concatenate([pooled, jnp.pad(d_logits, ((0, 0), (0, wide - classes)))], axis=1)
        d_top = jnp.pad(d_pooled / seq, ((0, 8 - batch), (0, 0)))
        g_in, g_out = backward(d_top, batch, xs, pre, w_in, w_out, layers - 1, layers)
        block_shape = (layers, -1) + g_out.shape[3:]
        red_in, red_out, head_all = sum_gradients(g_in, g_out.reshape(block_shape), head_part.reshape(16, -1), group_size)
        coef = jnp.stack([learn_rate, mom_coef])
        new_w_in, new_mom_in, new_w_out, new_mom_out, next_sums = update_forward(coef, x_next.reshape(-1, d), images, w_in, mom_in, red_in, w_out, mom_out, red_out.reshape(g_out.shape))
        head_rows = head_all.reshape(examples, d + wide)
        g_head = jnp.einsum('bd,bc->dc', head_rows[:, :d], head_rows[:, d:d + classes], preferred_element_type=F32)
        new_mom_head = mom_coef * mom_head + g_head
        new_w_head = w_head - learn_rate * new_mom_head
        next_pooled = (next_sums[:images] / seq).astype(BF16)
        logits_next = jnp.dot(next_pooled, new_w_head.astype(BF16), preferred_element_type=F32)
        return (logits_next, new_w_in, new_w_out, new_w_head, new_mom_in, new_mom_out, new_mom_head)

    return jax.shard_map(local_step, mesh=mesh, in_specs=(P(None, 'data', None, None), P(None, 'data'), P('data', None, None), P(), P(), P(), P(), P(), P(), P(), P()), out_specs=(P('data', None), P(), P(), P(), P(), P(), P()), check_vma=False)
```

```python
import functools

import jax
import jax.numpy as jnp
from jax import lax
from jax.experimental import pallas as pl
from jax.experimental.pallas import tpu as pltpu
from jax.sharding import PartitionSpec as P

LN_EPS = 1e-6
GELU_A = 0.7978845608028654
GELU_B = 0.044715
CHUNK = 512
UPD_CHUNK = 1024
FWD_CHUNK = 1024
RING = 4
LANES = 256
MESH_ID = pl.DeviceIdType.MESH
F32 = jnp.float32
BF16 = jnp.bfloat16


def norm_parts(x_f32):
    row_mean = jnp.mean(x_f32, axis=-1, keepdims=True)
    centered = x_f32 - row_mean
    row_var = jnp.mean(centered * centered, axis=-1, keepdims=True)
    inv = lax.rsqrt(row_var + LN_EPS)
    return centered * inv, inv


def gelu_tanh(pre):
    square = pre * pre
    half = 0.5 + 0.5 * jnp.tanh(pre * (GELU_A + (GELU_A * GELU_B) * square))
    return pre * half, half, square


def mm(a, b, dims=((1,), (0,))):
    return lax.dot_general(a, b, (dims, ((), ())), preferred_element_type=F32)


def image_sums(tok_act, images):
    rows = tok_act.shape[0]
    seq = rows // images
    start = lax.broadcasted_iota(jnp.int32, (16, rows), 0) * seq
    row = lax.broadcasted_iota(jnp.int32, (16, rows), 1)
    pick = ((row >= start) & (row < start + seq)).astype(F32).astype(BF16)
    return mm(pick, tok_act)


def cost(flops, bytes_accessed):
    return pl.CostEstimate(flops=flops, bytes_accessed=bytes_accessed, transcendentals=0)


def fwd_body(n_chunk, images, x0_ref, w1_ref, w2_ref, xs_ref, pre_ref, y_ref, x_s, n_s, acc_s):
    layer, step = pl.program_id(0), pl.program_id(1)

    @pl.when((layer == 0) & (step == 0))
    def _():
        x_s[...] = x0_ref[...]

    @pl.when(step == 0)
    def _():
        x_f32 = x_s[...].astype(F32)
        n_s[...] = norm_parts(x_f32)[0].astype(BF16)
        acc_s[...] = x_f32
        xs_ref[0] = x_s[...]

    pre = mm(n_s[...], w1_ref[0].astype(BF16))
    pre_ref[0] = pre
    hidden = gelu_tanh(pre)[0].astype(BF16)
    acc_s[...] += mm(hidden, w2_ref[0].astype(BF16))

    @pl.when(step == n_chunk - 1)
    def _():
        out = acc_s[...].astype(BF16)
        x_s[...] = out
        y_ref[...] = image_sums(out, images)


def forward(x0, images, w_in, w_out):
    layers, d, ff = w_in.shape
    rows = x0.shape[0]
    n_chunk = ff // FWD_CHUNK
    return pl.pallas_call(
        functools.partial(fwd_body, n_chunk, images),
        grid=(layers, n_chunk),
        in_specs=[
            pl.BlockSpec((rows, d), lambda l, j: (0, 0)),
            pl.BlockSpec((1, d, FWD_CHUNK), lambda l, j: (l, 0, j)),
            pl.BlockSpec((1, FWD_CHUNK, d), lambda l, j: (l, j, 0)),
        ],
        out_specs=[
            pl.BlockSpec((1, rows, d), lambda l, j: (l, 0, 0)),
            pl.BlockSpec((1, rows, FWD_CHUNK), lambda l, j: (l, 0, j)),
            pl.BlockSpec((16, d), lambda l, j: (0, 0)),
        ],
        out_shape=[
            jax.ShapeDtypeStruct((layers, rows, d), BF16),
            jax.ShapeDtypeStruct((layers, rows, ff), F32),
            jax.ShapeDtypeStruct((16, d), F32),
        ],
        scratch_shapes=[pltpu.VMEM((rows, d), BF16), pltpu.VMEM((rows, d), BF16), pltpu.VMEM((rows, d), F32)],
        cost_estimate=cost(4 * layers * rows * d * ff, 8 * layers * d * ff + 4 * layers * rows * ff),
        compiler_params=pltpu.CompilerParams(vmem_limit_bytes=48 << 20),
        name="mlp_forward",
    )(x0, w_in, w_out)


def backward_step(n_chunk, images, layer, step, slot_wait, slot_send, dtop_ref, xs_ref, pre_ref, w1_ref, w2_ref, g_s, d_s, db_s, n_s, dn_s):
    @pl.when((layer == 0) & (step == 0))
    def _():
        rows = d_s.shape[0]
        row = lax.broadcasted_iota(jnp.int32, d_s.shape, 0)
        value = jnp.broadcast_to(dtop_ref[0:1, :], d_s.shape)
        for image in range(1, images):
            value = jnp.where(row >= image * (rows // images), dtop_ref[image:image + 1, :], value)
        d_s[...] = value

    @pl.when(step == 0)
    def _():
        db_s[...] = d_s[...].astype(BF16)
        n_s[...] = norm_parts(xs_ref[0].astype(F32))[0].astype(BF16)
        dn_s[...] = jnp.zeros_like(dn_s)

    pre = pre_ref[0]
    gelu, half, square = gelu_tanh(pre)
    hidden = gelu.astype(BF16)
    slope = half + (pre * half) * ((1.0 - half) * (2.0 * GELU_A + (6.0 * GELU_A * GELU_B) * square))
    d_b = db_s[...]
    d_hidden = mm(d_b, w2_ref[0].astype(BF16), ((1,), (1,)))
    d_pre = (slope * d_hidden).astype(BF16)
    g_two = mm(hidden, d_b, ((0,), (0,))).astype(BF16)
    g_one = mm(n_s[...], d_pre, ((0,), (0,))).astype(BF16)
    slot = slot_wait()
    for part in range(2):
        g_s[slot, part] = g_one[:, part * LANES:(part + 1) * LANES]
        g_s[slot, 2 + part] = g_two[:, part * LANES:(part + 1) * LANES]
    slot_send()
    dn_s[...] += mm(d_pre, w1_ref[0].astype(BF16), ((1,), (1,)))

    @pl.when(step == n_chunk - 1)
    def _():
        normed, inv = norm_parts(xs_ref[0].astype(F32))
        dn = dn_s[...]
        along = jnp.mean(dn * normed, axis=-1, keepdims=True)
        out = d_s[...] + inv * (dn - jnp.mean(dn, axis=-1, keepdims=True) - normed * along)
        d_s[...] = out


def next_body(n_chunk, images, coef_ref, x0_ref, w1_ref, m1_ref, g1_ref, w2_ref, m2_ref, g2_ref,
              nw1_ref, nm1_ref, nw2_ref, nm2_ref, y_ref, x_s, n_s, acc_s):
    layer, step = pl.program_id(0), pl.program_id(1)
    rate, momentum = coef_ref[0], coef_ref[1]

    @pl.when((layer == 0) & (step == 0))
    def _():
        x_s[...] = x0_ref[...]

    @pl.when(step == 0)
    def _():
        x_f32 = x_s[...].astype(F32)
        n_s[...] = norm_parts(x_f32)[0].astype(BF16)
        acc_s[...] = x_f32

    g_one = jnp.concatenate([g1_ref[0, 0], g1_ref[0, 1], g1_ref[0, 2], g1_ref[0, 3]], axis=1)
    g_two = jnp.concatenate([jnp.concatenate([g2_ref[0, 0, r], g2_ref[0, 1, r]], axis=1) for r in range(2)], axis=0)
    m1 = momentum * m1_ref[0] + g_one.astype(F32)
    w1 = w1_ref[0] - rate * m1
    nm1_ref[0] = m1
    nw1_ref[0] = w1
    m2 = momentum * m2_ref[0] + g_two.astype(F32)
    w2 = w2_ref[0] - rate * m2
    nm2_ref[0] = m2
    nw2_ref[0] = w2
    pre = mm(n_s[...], w1.astype(BF16))
    hidden = gelu_tanh(pre)[0].astype(BF16)
    acc_s[...] += mm(hidden, w2.astype(BF16))

    @pl.when(step == n_chunk - 1)
    def _():
        out = acc_s[...].astype(BF16)
        x_s[...] = out
        y_ref[...] = image_sums(out, images)


def update_forward(coef, x0, images, w_in, mom_in, g_in, w_out, mom_out, g_out):
    layers, d, ff = w_in.shape
    rows = x0.shape[0]
    n_chunk = ff // UPD_CHUNK
    in_block = pl.BlockSpec((1, d, UPD_CHUNK), lambda l, j: (l, 0, j))
    out_block = pl.BlockSpec((1, UPD_CHUNK, d), lambda l, j: (l, j, 0))
    return pl.pallas_call(
        functools.partial(next_body, n_chunk, images),
        grid=(layers, n_chunk),
        in_specs=[
            pl.BlockSpec(memory_space=pltpu.SMEM),
            pl.BlockSpec((rows, d), lambda l, j: (0, 0)),
            in_block,
            in_block,
            pl.BlockSpec((1, 4, d, LANES), lambda l, j: (l, j, 0, 0)),
            out_block,
            out_block,
            pl.BlockSpec((1, 2, 2, 512, LANES), lambda l, j: (l, 0, j, 0, 0)),
        ],
        out_specs=[in_block, in_block, out_block, out_block, pl.BlockSpec((16, d), lambda l, j: (0, 0))],
        out_shape=[
            jax.ShapeDtypeStruct(w_in.shape, F32),
            jax.ShapeDtypeStruct(w_in.shape, F32),
            jax.ShapeDtypeStruct(w_out.shape, F32),
            jax.ShapeDtypeStruct(w_out.shape, F32),
            jax.ShapeDtypeStruct((16, d), F32),
        ],
        scratch_shapes=[pltpu.VMEM((rows, d), BF16), pltpu.VMEM((rows, d), BF16), pltpu.VMEM((rows, d), F32)],
        cost_estimate=cost(4 * layers * rows * d * ff, 36 * layers * d * ff),
        compiler_params=pltpu.CompilerParams(vmem_limit_bytes=60 << 20),
        name="update_forward",
    )(coef, x0, w_in, mom_in, g_in, w_out, mom_out, g_out)


def backward_sum_body(layers, n_chunk, images, dtop_ref, xs_ref, pre_ref, w1_ref, w2_ref, head_ref, o1_ref, o2_ref, all_ref, g1_ref, g2_ref,
                      g_s, d_s, db_s, n_s, dn_s, work, land0, land1, land2, land3, turn, head,
                      g_sem, load_sem, d0_send, d0_recv, ring_send, ring_recv, d1_send, d1_recv, out_sem, head_send, head_recv, head_sem, credit):
    layer_index, step_index = pl.program_id(0), pl.program_id(1)
    grid_step = layer_index * n_chunk + step_index
    n = RING
    rows = work.shape[2]
    sub = (rows, rows // n, rows // (n * n))
    me = lax.axis_index('data')
    core = lax.rem(me, 2)
    partner = me + 1 - 2 * core
    own, other = core * n, (1 - core) * n
    strides = (2, 2 * n, 2 * n * n)
    pos = [lax.rem(lax.div(me, stride), n) for stride in strides]
    near = [me + (1 - 2 * lax.rem(p, 2)) * stride for p, stride in zip(pos, strides)]
    far = [me + (3 - 2 * p) * stride for p, stride in zip(pos, strides)]
    near_bit = [lax.rem(lax.div(p + 1, 2), 2) for p in pos]
    far_bit = [lax.div(p, 2) for p in pos]

    barrier = pltpu.get_barrier_semaphore()
    greeted = [partner] + near + far

    @pl.when(grid_step == 0)
    def _():
        for device in greeted:
            pl.semaphore_signal(barrier, inc=1, device_id=(device,), device_id_type=MESH_ID)
        pl.semaphore_wait(barrier, len(greeted))

    def each(wave, fn):
        for colour in range(3):
            for kind in range(2):
                layer = colour + 3 * wave
                fn((g1_ref, g2_ref)[kind], (o1_ref, o2_ref)[kind], kind * layers + layer, layer, colour, (wave + kind) % 2)

    def remote(src, dst, send, recv, device):
        return pltpu.make_async_remote_copy(src_ref=src, dst_ref=dst, send_sem=send, recv_sem=recv, device_id=(device,), device_id_type=MESH_ID)

    def mix(a, b, flip):
        return a + flip * (b - a)

    def bits(colour, flip, stage):
        axis = (colour + stage - 1) % 3
        return mix(near_bit[axis], far_bit[axis], flip), mix(far_bit[axis], near_bit[axis], flip)

    def unit(colour, flip, stage):
        hi, lo = bits(colour, flip, stage)
        return 2 * hi + lo

    def units(m, colour, flip, stage, first, count):
        if stage == 1:
            return work.at[m, pl.ds(first, count)]
        row = first * sub[stage - 1]
        if stage == 3:
            row = row + unit(colour, flip, 2) * sub[1]
        row = pl.multiple_of(row, sub[stage - 1])
        return work.at[m, pl.ds(unit(colour, flip, 1), 1), pl.ds(row, count * sub[stage - 1])]

    def land(m, stage, step):
        first, count = ((0, 2), (2, 1))[step]
        if stage == 1:
            return land1.at[m, pl.ds(first, count)]
        size = sub[stage - 1]
        return (land2, land3)[stage - 2].at[pl.ds(m, 1), pl.ds(first * size, count * size)]

    def land_unit(m, which):
        return land3.at[pl.ds(m, 1), pl.ds(pl.multiple_of(which * sub[2], sub[2]), sub[2])]

    def copies(t, m, colour, flip):
        scatter = t < 6
        stage = t // 2 + 1 if scatter else 6 - t // 2
        step = t % 2
        hi, lo = bits(colour, flip, stage)
        axis = (colour + stage - 1) % 3
        with_first = (step == 0) == scatter
        to = mix(near[axis], far[axis], flip) if with_first else mix(far[axis], near[axis], flip)
        kept = (2 * hi, 2) if with_first else (2 * hi + lo, 1)
        given = (2 - 2 * hi, 2) if with_first else (2 * hi + 1 - lo, 1)
        if scatter:
            src = turn.at[pl.ds(m, 1)] if t == 5 else units(m, colour, flip, stage, *given)
            return src, land(m, stage, step), land(m, stage, step), to, kept
        src = units(m, colour, flip, stage, *kept)
        return src, src, units(m, colour, flip, stage, *given), to, given

    def message(t, m, colour, flip):
        src, dst, _, to, _ = copies(t, m, colour, flip)
        return remote(src, dst, ring_send.at[m], ring_recv.at[m, t], to)

    def arrival(t, m, colour, flip):
        _, _, here, to, _ = copies(t, m, colour, flip)
        return remote(here, here, ring_send.at[m], ring_recv.at[m, t], to)

    def pair(colour, flip, k):
        hi, _ = bits(colour, flip, 1)
        return mix(2 - 2 * hi, 2 * hi, k)

    def cell(m):
        return m // layers * 3 + m % 3

    def load_copy(g_ref, m, layer, colour, flip, k):
        first = pair(colour, flip, k)
        return pltpu.make_async_copy(g_ref.at[layer, pl.ds(own + first, 2)], work.at[m, pl.ds(first, 2)], load_sem.at[m, k])

    def swap_copy(g_ref, m, layer, colour, flip, k):
        first = pair(colour, flip, k)
        return remote(g_ref.at[layer, pl.ds(other + first, 2)], land0.at[cell(m), pl.ds(first, 2)], d0_send.at[m, k], d0_recv.at[m, k], partner)

    def final(colour, flip, k):
        hi, lo = bits(colour, flip, 1)
        return ((2 * hi + lo, 1), (2 * hi + 1 - lo, 1), (2 - 2 * hi, 2))[k]

    def share_copy(o_ref, m, layer, colour, flip, k, half):
        first, count = final(colour, flip, k)
        return remote(work.at[m, pl.ds(first, count)], o_ref.at[layer, pl.ds(half + first, count)], d1_send.at[m, k], d1_recv.at[m, k], partner)

    def out_copy(o_ref, m, layer, colour, flip, k):
        first, count = final(colour, flip, k)
        return pltpu.make_async_copy(work.at[m, pl.ds(first, count)], o_ref.at[layer, pl.ds(own + first, count)], out_sem.at[m, k])

    def accumulate(dst, sources):
        blocks, count, _ = dst.shape
        step = min(count, 64)

        @pl.loop(0, count // step)
        def _(r):
            part = pl.ds(pl.multiple_of(r * step, step), step)
            for block in range(blocks):
                total = sources[0][block, part, :].astype(F32)
                for source in sources[1:]:
                    total = total + source[block, part, :].astype(F32)
                dst[block, part, :] = total.astype(BF16)

    head_way = 1 - 2 * core

    def head_message(j, back):
        axis, s = divmod(j, n - 1)
        index = lax.rem(pos[axis] - head_way * (s + back) + 2 * n, n)
        to = me + (lax.rem(pos[axis] + head_way + n, n) - pos[axis]) * strides[axis]
        if axis == 0:
            part = head.at[core, pos[2], pos[1], index]
        elif axis == 1:
            part = head.at[core, pos[2], index]
        else:
            part = head.at[core, index]
        return remote(part, part, head_send, head_recv.at[j], to)

    def head_share(which):
        return remote(head.at[which], head.at[which], head_send, head_recv.at[3 * (n - 1)], partner)

    def head_tick(t):
        count = 3 * (n - 1)
        if t == 0:
            first = pltpu.make_async_copy(head_ref, head.at[core, pos[2], pos[1], pos[0]], head_sem)
            first.start()
            first.wait()
        elif t <= count:
            head_message(t - 1, 1).wait_recv()
            head_message(t - 1, 0).wait_send()
        if t < count:
            head_message(t, 0).start()
        elif t == count:
            head_share(core).start()

    def begin(wave):
        for k in range(2):
            def body(g_ref, o_ref, m, layer, colour, flip, k=k):
                swap_copy(g_ref, m, layer, colour, flip, k).start()
                load_copy(g_ref, m, layer, colour, flip, k).start()
            each(wave, body)

    def tick(wave, t):
        def body(g_ref, o_ref, m, layer, colour, flip):
            if t > 0:
                arrival(t - 1, m, colour, flip).wait_recv()
                message(t - 1, m, colour, flip).wait_send()
            if t < 2:
                load_copy(g_ref, m, layer, colour, flip, t).wait()
                swap_copy(g_ref, m, layer, colour, flip, t).wait_recv()
                blocks = units(m, colour, flip, 1, pair(colour, flip, t), 2)
                sources = [land0.at[cell(m), pl.ds(pair(colour, flip, t), 2)]] + ([land(m, 1, 0)] if t > 0 else [])
                accumulate(blocks, [blocks] + sources)
            elif t == 5:
                hi, lo = bits(colour, flip, 3)
                mine, theirs = units(m, colour, flip, 3, 2 * hi + lo, 1), units(m, colour, flip, 3, 2 * hi + 1 - lo, 1)
                accumulate(turn.at[pl.ds(m, 1)], [theirs, land_unit(m, 1 - lo)])
                accumulate(mine, [mine, land_unit(m, lo)])
            elif t < 7:
                _, _, here, _, kept = copies(t - 1, m, colour, flip)
                blocks = units(m, colour, flip, (t + 1) // 2, *kept)
                accumulate(blocks, [blocks, here])
            if t < 12:
                message(t, m, colour, flip).start()
            k = t - 10
            if k >= 0:
                share_copy(o_ref, m, layer, colour, flip, k, own).start()
                out_copy(o_ref, m, layer, colour, flip, k).start()
        each(wave, body)

    def finish(wave):
        def body(g_ref, o_ref, m, layer, colour, flip):
            for k in range(3):
                share_copy(o_ref, m, layer, colour, flip, k, own).wait_send()
                share_copy(o_ref, m, layer, colour, flip, k, other).wait_recv()
                out_copy(o_ref, m, layer, colour, flip, k).wait()
            for k in range(2):
                swap_copy(g_ref, m, layer, colour, flip, k).wait_send()
        each(wave, body)

    real_layer = layers - 1 - layer_index
    slot = lax.rem(step_index, 2)

    def slot_copies(which, at_step):
        blocks = [(g1_ref, 2 * at_step), (g1_ref, 2 * at_step + 1), (g2_ref, at_step), (g2_ref, n_chunk + at_step)]
        return [pltpu.make_async_copy(g_s.at[which, q], ref.at[real_layer, block], g_sem.at[which, q]) for q, (ref, block) in enumerate(blocks)]

    def slot_wait():
        @pl.when(step_index >= 2)
        def _():
            for copy in slot_copies(slot, step_index - 2):
                copy.wait()
        return slot

    def slot_send():
        for copy in slot_copies(slot, step_index):
            copy.start()

    backward_step(n_chunk, images, layer_index, step_index, slot_wait, slot_send, dtop_ref, xs_ref, pre_ref, w1_ref, w2_ref, g_s, d_s, db_s, n_s, dn_s)

    @pl.when(step_index == n_chunk - 1)
    def _():
        for past in (1, 0):
            for copy in slot_copies((n_chunk - 1 - past) % 2, n_chunk - 1 - past):
                copy.wait()

    half_way = layers // 2 * n_chunk
    plan = {half_way - 1: [lambda: begin(1)]}
    for offset, t in ((0, 0), (4, 1), (6, 2), (8, 3), (9, 4), (10, 5), (11, 6)):
        plan.setdefault(half_way + offset, []).append(functools.partial(tick, 1, t))
    plan[half_way + 4].append(lambda: pl.semaphore_signal(credit, inc=1, device_id=(partner,), device_id_type=MESH_ID))
    for t in range(3 * (n - 1) + 1):
        plan.setdefault(half_way + t, []).append(functools.partial(head_tick, t))
    rest = [lambda: pl.semaphore_wait(credit, 1), lambda: begin(0)]
    for wave, t in ((1, 7), (1, 8), (0, 0), (1, 9), (0, 1), (1, 10), (0, 2), (0, 3), (1, 11), (0, 4), (0, 5), (0, 6), (0, 7), (1, 12), (0, 8), (0, 9), (0, 10), (0, 11), (0, 12)):
        rest.append(functools.partial(tick, wave, t))
    plan[2 * half_way - 1] += rest
    for when, actions in plan.items():
        @pl.when(grid_step == when)
        def _(actions=actions):
            for action in actions:
                action()

    @pl.when(grid_step == 2 * half_way - 1)
    def _():
        head_share(1 - core).wait_recv()
        head_share(core).wait_send()
        head_out = pltpu.make_async_copy(head, all_ref, head_sem)
        head_out.start()
        finish(1)
        finish(0)
        head_out.wait()


def backward_sum(d_top, images, xs, pre, w_in, w_out, head_part, group_size):
    n = RING
    if group_size != 2 * n ** 3:
        raise ValueError("needs a 4x4x4 torus")
    layers, d, ff = w_in.shape
    rows = xs.shape[1]
    n_chunk = ff // CHUNK
    count = 2 * layers
    size = CHUNK
    dma = pltpu.SemaphoreType.DMA
    head_shape = (2, n, n, n) + head_part.shape
    sums = jax.ShapeDtypeStruct((layers, 2 * n, size, LANES), BF16)
    last = layers - 1
    return pl.pallas_call(
        functools.partial(backward_sum_body, layers, n_chunk, images),
        grid=(layers, n_chunk),
        in_specs=[
            pl.BlockSpec(d_top.shape, lambda l, j: (0, 0)),
            pl.BlockSpec((1, rows, d), lambda l, j: (last - l, 0, 0)),
            pl.BlockSpec((1, rows, CHUNK), lambda l, j: (last - l, 0, j)),
            pl.BlockSpec((1, d, CHUNK), lambda l, j: (last - l, 0, j)),
            pl.BlockSpec((1, CHUNK, d), lambda l, j: (last - l, j, 0)),
            pl.BlockSpec(memory_space=pl.ANY),
        ],
        out_specs=[pl.BlockSpec(memory_space=pl.ANY)] * 5,
        out_shape=[sums, sums, jax.ShapeDtypeStruct(head_shape, BF16), sums, sums],
        scratch_shapes=[
            pltpu.VMEM((2, 4, size, LANES), BF16),
            pltpu.VMEM((rows, d), F32),
            pltpu.VMEM((rows, d), BF16),
            pltpu.VMEM((rows, d), BF16),
            pltpu.VMEM((rows, d), F32),
            pltpu.VMEM((count, n, size, LANES), BF16),
            pltpu.VMEM((6, n, size, LANES), BF16),
            pltpu.VMEM((count, 3, size, LANES), BF16),
            pltpu.VMEM((count, 3 * size // n, LANES), BF16),
            pltpu.VMEM((count, 3 * size // (n * n), LANES), BF16),
            pltpu.VMEM((count, size // (n * n), LANES), BF16),
            pltpu.VMEM(head_shape, BF16),
            dma((2, 4)),
            dma((count, 2)),
            dma((count, 2)),
            dma((count, 2)),
            dma((count,)),
            dma((count, 12)),
            dma((count, 3)),
            dma((count, 3)),
            dma((count, 3)),
            dma,
            dma((3 * (n - 1) + 1,)),
            dma,
            pltpu.SemaphoreType.REGULAR,
        ],
        cost_estimate=cost(8 * layers * rows * d * ff, layers * (12 * d * ff + 4 * rows * ff)),
        compiler_params=pltpu.CompilerParams(collective_id=0, has_side_effects=True, vmem_limit_bytes=63 << 20),
        name="backward_sum",
    )(d_top, xs, pre, w_in, w_out, head_part)


def head_backward(pooled, lab_row, w_head_b, examples):
    logits = jnp.dot(pooled, w_head_b, preferred_element_type=F32)
    soft_prob = jax.nn.softmax(logits, axis=-1)
    onehot = (lab_row[:, None] == jnp.arange(logits.shape[1])[None, :]).astype(F32)
    d_logits = ((soft_prob - onehot) / examples).astype(BF16)
    d_pooled = jnp.einsum('bc,dc->bd', d_logits, w_head_b, preferred_element_type=F32)
    return d_logits, d_pooled


def solution(mesh):
    group_size = mesh.shape['data']

    def local_step(x_step, labels, x_next, w_in, w_out, w_head, mom_in, mom_out, mom_head, learn_rate, mom_coef):
        micro_count, images, seq, d = x_step.shape
        layers = w_in.shape[0]
        classes = w_head.shape[1]
        batch = micro_count * images
        examples = batch * group_size
        xs, pre, sums = forward(x_step.reshape(-1, d), batch, w_in, w_out)
        pooled = (sums[:batch] / seq).astype(BF16)
        d_logits, d_pooled = head_backward(pooled, labels.reshape(-1), w_head.astype(BF16), examples)
        wide = -(-classes // 512) * 512
        head_part = jnp.concatenate([pooled, jnp.pad(d_logits, ((0, 0), (0, wide - classes)))], axis=1)
        d_top = jnp.pad(d_pooled / seq, ((0, 8 - batch), (0, 0)))
        red_in, red_out, head_all, _, _ = backward_sum(d_top, batch, xs, pre, w_in, w_out, head_part.reshape(16, -1), group_size)
        coef = jnp.stack([learn_rate, mom_coef])
        new_w_in, new_mom_in, new_w_out, new_mom_out, next_sums = update_forward(coef, x_next.reshape(-1, d), images, w_in, mom_in, red_in, w_out, mom_out, red_out.reshape(layers, 2, -1, CHUNK, LANES))
        head_rows = head_all.reshape(examples, d + wide)
        g_head = jnp.einsum('bd,bc->dc', head_rows[:, :d], head_rows[:, d:d + classes], preferred_element_type=F32)
        new_mom_head = mom_coef * mom_head + g_head
        new_w_head = w_head - learn_rate * new_mom_head
        next_pooled = (next_sums[:images] / seq).astype(BF16)
        logits_next = jnp.dot(next_pooled, new_w_head.astype(BF16), preferred_element_type=F32)
        return (logits_next, new_w_in, new_w_out, new_w_head, new_mom_in, new_mom_out, new_mom_head)

    return jax.shard_map(local_step, mesh=mesh, in_specs=(P(None, 'data', None, None), P(None, 'data'), P('data', None, None), P(), P(), P(), P(), P(), P(), P(), P()), out_specs=(P('data', None), P(), P(), P(), P(), P(), P()), check_vma=False)
```

```python
import functools

import jax
import jax.numpy as jnp
from jax import lax
from jax.experimental import pallas as pl
from jax.experimental.pallas import tpu as pltpu
from jax.sharding import PartitionSpec as P

LN_EPS = 1e-6
GELU_A = 0.7978845608028654
GELU_B = 0.044715
CHUNK = 512
UPD_CHUNK = 1024
FWD_CHUNK = 2048
RING = 4
LANES = 256
MESH_ID = pl.DeviceIdType.MESH
F32 = jnp.float32
BF16 = jnp.bfloat16


def norm_parts(x_f32):
    row_mean = jnp.mean(x_f32, axis=-1, keepdims=True)
    centered = x_f32 - row_mean
    row_var = jnp.mean(centered * centered, axis=-1, keepdims=True)
    inv = lax.rsqrt(row_var + LN_EPS)
    return centered * inv, inv


def gelu_tanh(pre):
    square = pre * pre
    half = 0.5 + 0.5 * jnp.tanh(pre * (GELU_A + (GELU_A * GELU_B) * square))
    return pre * half, half, square


def mm(a, b, dims=((1,), (0,))):
    return lax.dot_general(a, b, (dims, ((), ())), preferred_element_type=F32)


def image_sums(tok_act, images):
    rows = tok_act.shape[0]
    seq = rows // images
    start = lax.broadcasted_iota(jnp.int32, (16, rows), 0) * seq
    row = lax.broadcasted_iota(jnp.int32, (16, rows), 1)
    pick = ((row >= start) & (row < start + seq)).astype(F32).astype(BF16)
    return mm(pick, tok_act)


def cost(flops, bytes_accessed):
    return pl.CostEstimate(flops=flops, bytes_accessed=bytes_accessed, transcendentals=0)


def fwd_body(n_chunk, images, x0_ref, w1_ref, w2_ref, xs_ref, pre_ref, y_ref, x_s, n_s, acc_s):
    layer, step = pl.program_id(0), pl.program_id(1)

    @pl.when((layer == 0) & (step == 0))
    def _():
        x_s[...] = x0_ref[...]

    @pl.when(step == 0)
    def _():
        x_f32 = x_s[...].astype(F32)
        n_s[...] = norm_parts(x_f32)[0].astype(BF16)
        acc_s[...] = x_f32
        xs_ref[0] = x_s[...]

    pre = mm(n_s[...], w1_ref[0].astype(BF16))
    pre_ref[0] = pre
    hidden = gelu_tanh(pre)[0].astype(BF16)
    acc_s[...] += mm(hidden, w2_ref[0].astype(BF16))

    @pl.when(step == n_chunk - 1)
    def _():
        out = acc_s[...].astype(BF16)
        x_s[...] = out
        y_ref[...] = image_sums(out, images)


def forward(x0, images, w_in, w_out):
    layers, d, ff = w_in.shape
    rows = x0.shape[0]
    n_chunk = ff // FWD_CHUNK
    return pl.pallas_call(
        functools.partial(fwd_body, n_chunk, images),
        grid=(layers, n_chunk),
        in_specs=[
            pl.BlockSpec((rows, d), lambda l, j: (0, 0)),
            pl.BlockSpec((1, d, FWD_CHUNK), lambda l, j: (l, 0, j)),
            pl.BlockSpec((1, FWD_CHUNK, d), lambda l, j: (l, j, 0)),
        ],
        out_specs=[
            pl.BlockSpec((1, rows, d), lambda l, j: (l, 0, 0)),
            pl.BlockSpec((1, rows, FWD_CHUNK), lambda l, j: (l, 0, j)),
            pl.BlockSpec((16, d), lambda l, j: (0, 0)),
        ],
        out_shape=[
            jax.ShapeDtypeStruct((layers, rows, d), BF16),
            jax.ShapeDtypeStruct((layers, rows, ff), F32),
            jax.ShapeDtypeStruct((16, d), F32),
        ],
        scratch_shapes=[pltpu.VMEM((rows, d), BF16), pltpu.VMEM((rows, d), BF16), pltpu.VMEM((rows, d), F32)],
        cost_estimate=cost(4 * layers * rows * d * ff, 8 * layers * d * ff + 4 * layers * rows * ff),
        compiler_params=pltpu.CompilerParams(vmem_limit_bytes=62 << 20),
        name="mlp_forward",
    )(x0, w_in, w_out)


def bwd_body(n_chunk, images, dtop_ref, xs_ref, pre_ref, w1_ref, w2_ref, g1_ref, g2_ref, d_s, db_s, n_s, dn_s):
    layer, step = pl.program_id(0), pl.program_id(1)

    @pl.when((layer == 0) & (step == 0))
    def _():
        rows = d_s.shape[0]
        row = lax.broadcasted_iota(jnp.int32, d_s.shape, 0)
        value = jnp.broadcast_to(dtop_ref[0:1, :], d_s.shape)
        for image in range(1, images):
            value = jnp.where(row >= image * (rows // images), dtop_ref[image:image + 1, :], value)
        d_s[...] = value

    @pl.when(step == 0)
    def _():
        db_s[...] = d_s[...].astype(BF16)
        n_s[...] = norm_parts(xs_ref[0].astype(F32))[0].astype(BF16)
        dn_s[...] = jnp.zeros_like(dn_s)

    pre = pre_ref[0]
    gelu, half, square = gelu_tanh(pre)
    hidden = gelu.astype(BF16)
    slope = half + (pre * half) * ((1.0 - half) * (2.0 * GELU_A + (6.0 * GELU_A * GELU_B) * square))
    d_b = db_s[...]
    d_hidden = mm(d_b, w2_ref[0].astype(BF16), ((1,), (1,)))
    d_pre = (slope * d_hidden).astype(BF16)
    g_two = mm(hidden, d_b, ((0,), (0,))).astype(BF16)
    g_one = mm(n_s[...], d_pre, ((0,), (0,))).astype(BF16)
    for part in range(2):
        g1_ref[0, part] = g_one[:, part * LANES:(part + 1) * LANES]
        g2_ref[0, part, 0] = g_two[:, part * LANES:(part + 1) * LANES]
    dn_s[...] += mm(d_pre, w1_ref[0].astype(BF16), ((1,), (1,)))

    @pl.when(step == n_chunk - 1)
    def _():
        normed, inv = norm_parts(xs_ref[0].astype(F32))
        dn = dn_s[...]
        along = jnp.mean(dn * normed, axis=-1, keepdims=True)
        out = d_s[...] + inv * (dn - jnp.mean(dn, axis=-1, keepdims=True) - normed * along)
        d_s[...] = out


def backward(d_top, images, xs, pre, w_in, w_out, first, count):
    _, d, ff = w_in.shape
    rows = xs.shape[1]
    n_chunk = ff // CHUNK
    return pl.pallas_call(
        functools.partial(bwd_body, n_chunk, images),
        grid=(count, n_chunk),
        in_specs=[
            pl.BlockSpec(d_top.shape, lambda l, j: (0, 0)),
            pl.BlockSpec((1, rows, d), lambda l, j: (first - l, 0, 0)),
            pl.BlockSpec((1, rows, CHUNK), lambda l, j: (first - l, 0, j)),
            pl.BlockSpec((1, d, CHUNK), lambda l, j: (first - l, 0, j)),
            pl.BlockSpec((1, CHUNK, d), lambda l, j: (first - l, j, 0)),
        ],
        out_specs=[
            pl.BlockSpec((1, 2, d, LANES), lambda l, j: (first - l, j, 0, 0)),
            pl.BlockSpec((1, 2, 1, CHUNK, LANES), lambda l, j: (first - l, 0, j, 0, 0)),
        ],
        out_shape=[
            jax.ShapeDtypeStruct((count, 2 * n_chunk, d, LANES), BF16),
            jax.ShapeDtypeStruct((count, 2, n_chunk, CHUNK, LANES), BF16),
        ],
        scratch_shapes=[
            pltpu.VMEM((rows, d), F32),
            pltpu.VMEM((rows, d), BF16),
            pltpu.VMEM((rows, d), BF16),
            pltpu.VMEM((rows, d), F32),
        ],
        cost_estimate=cost(8 * count * rows * d * ff, count * (12 * d * ff + 4 * rows * ff)),
        compiler_params=pltpu.CompilerParams(vmem_limit_bytes=62 << 20),
        name="mlp_backward",
    )(d_top, xs, pre, w_in, w_out)


def next_body(n_chunk, images, coef_ref, x0_ref, w1_ref, m1_ref, g1_ref, w2_ref, m2_ref, g2_ref,
              nw1_ref, nm1_ref, nw2_ref, nm2_ref, y_ref, x_s, n_s, acc_s):
    layer, step = pl.program_id(0), pl.program_id(1)
    rate, momentum = coef_ref[0], coef_ref[1]

    @pl.when((layer == 0) & (step == 0))
    def _():
        x_s[...] = x0_ref[...]

    @pl.when(step == 0)
    def _():
        x_f32 = x_s[...].astype(F32)
        n_s[...] = norm_parts(x_f32)[0].astype(BF16)
        acc_s[...] = x_f32

    g_one = jnp.concatenate([g1_ref[0, 0], g1_ref[0, 1], g1_ref[0, 2], g1_ref[0, 3]], axis=1)
    g_two = jnp.concatenate([jnp.concatenate([g2_ref[0, 0, r], g2_ref[0, 1, r]], axis=1) for r in range(2)], axis=0)
    m1 = momentum * m1_ref[0] + g_one.astype(F32)
    w1 = w1_ref[0] - rate * m1
    nm1_ref[0] = m1
    nw1_ref[0] = w1
    m2 = momentum * m2_ref[0] + g_two.astype(F32)
    w2 = w2_ref[0] - rate * m2
    nm2_ref[0] = m2
    nw2_ref[0] = w2
    pre = mm(n_s[...], w1.astype(BF16))
    hidden = gelu_tanh(pre)[0].astype(BF16)
    acc_s[...] += mm(hidden, w2.astype(BF16))

    @pl.when(step == n_chunk - 1)
    def _():
        out = acc_s[...].astype(BF16)
        x_s[...] = out
        y_ref[...] = image_sums(out, images)


def update_forward(coef, x0, images, w_in, mom_in, g_in, w_out, mom_out, g_out):
    layers, d, ff = w_in.shape
    rows = x0.shape[0]
    n_chunk = ff // UPD_CHUNK
    in_block = pl.BlockSpec((1, d, UPD_CHUNK), lambda l, j: (l, 0, j))
    out_block = pl.BlockSpec((1, UPD_CHUNK, d), lambda l, j: (l, j, 0))
    return pl.pallas_call(
        functools.partial(next_body, n_chunk, images),
        grid=(layers, n_chunk),
        in_specs=[
            pl.BlockSpec(memory_space=pltpu.SMEM),
            pl.BlockSpec((rows, d), lambda l, j: (0, 0)),
            in_block,
            in_block,
            pl.BlockSpec((1, 4, d, LANES), lambda l, j: (l, j, 0, 0)),
            out_block,
            out_block,
            pl.BlockSpec((1, 2, 2, 512, LANES), lambda l, j: (l, 0, j, 0, 0)),
        ],
        out_specs=[in_block, in_block, out_block, out_block, pl.BlockSpec((16, d), lambda l, j: (0, 0))],
        out_shape=[
            jax.ShapeDtypeStruct(w_in.shape, F32),
            jax.ShapeDtypeStruct(w_in.shape, F32),
            jax.ShapeDtypeStruct(w_out.shape, F32),
            jax.ShapeDtypeStruct(w_out.shape, F32),
            jax.ShapeDtypeStruct((16, d), F32),
        ],
        scratch_shapes=[pltpu.VMEM((rows, d), BF16), pltpu.VMEM((rows, d), BF16), pltpu.VMEM((rows, d), F32)],
        cost_estimate=cost(4 * layers * rows * d * ff, 36 * layers * d * ff),
        compiler_params=pltpu.CompilerParams(vmem_limit_bytes=60 << 20),
        name="update_forward",
    )(coef, x0, w_in, mom_in, g_in, w_out, mom_out, g_out)


def sum_body(layers, g1_ref, g2_ref, head_ref, o1_ref, o2_ref, all_ref, work, land0, land1, land2, land3, turn, head,
             load_sem, d0_send, d0_recv, ring_send, ring_recv, d1_send, d1_recv, out_sem, head_send, head_recv, head_sem):
    n = RING
    rows = work.shape[2]
    sub = (rows, rows // n, rows // (n * n))
    me = lax.axis_index('data')
    core = lax.rem(me, 2)
    partner = me + 1 - 2 * core
    own, other = core * n, (1 - core) * n
    strides = (2, 2 * n, 2 * n * n)
    pos = [lax.rem(lax.div(me, stride), n) for stride in strides]
    near = [me + (1 - 2 * lax.rem(p, 2)) * stride for p, stride in zip(pos, strides)]
    far = [me + (3 - 2 * p) * stride for p, stride in zip(pos, strides)]
    near_bit = [lax.rem(lax.div(p + 1, 2), 2) for p in pos]
    far_bit = [lax.div(p, 2) for p in pos]

    barrier = pltpu.get_barrier_semaphore()
    greeted = [partner] + near + far
    for device in greeted:
        pl.semaphore_signal(barrier, inc=1, device_id=(device,), device_id_type=MESH_ID)
    pl.semaphore_wait(barrier, len(greeted))

    def each(fn):
        @pl.loop(0, layers // 3)
        def _(i):
            for colour in range(3):
                for kind in range(2):
                    flip = lax.rem(i + kind, 2)
                    layer = colour + 3 * i
                    fn((g1_ref, g2_ref)[kind], (o1_ref, o2_ref)[kind], kind * layers + layer, layer, colour, flip)

    def remote(src, dst, send, recv, device):
        return pltpu.make_async_remote_copy(src_ref=src, dst_ref=dst, send_sem=send, recv_sem=recv, device_id=(device,), device_id_type=MESH_ID)

    def mix(a, b, flip):
        return a + flip * (b - a)

    def bits(colour, flip, stage):
        axis = (colour + stage - 1) % 3
        return mix(near_bit[axis], far_bit[axis], flip), mix(far_bit[axis], near_bit[axis], flip)

    def unit(colour, flip, stage):
        hi, lo = bits(colour, flip, stage)
        return 2 * hi + lo

    def units(m, colour, flip, stage, first, count):
        if stage == 1:
            return work.at[m, pl.ds(own + first, count)]
        row = first * sub[stage - 1]
        if stage == 3:
            row = row + unit(colour, flip, 2) * sub[1]
        row = pl.multiple_of(row, sub[stage - 1])
        return work.at[m, pl.ds(own + unit(colour, flip, 1), 1), pl.ds(row, count * sub[stage - 1])]

    def land(m, stage, step):
        first, count = ((0, 2), (2, 1))[step]
        if stage == 1:
            return land1.at[m, pl.ds(first, count)]
        size = sub[stage - 1]
        return (land2, land3)[stage - 2].at[pl.ds(m, 1), pl.ds(first * size, count * size)]

    def land_unit(m, which):
        return land3.at[pl.ds(m, 1), pl.ds(pl.multiple_of(which * sub[2], sub[2]), sub[2])]

    def copies(t, m, colour, flip):
        scatter = t < 6
        stage = t // 2 + 1 if scatter else 6 - t // 2
        step = t % 2
        hi, lo = bits(colour, flip, stage)
        axis = (colour + stage - 1) % 3
        with_first = (step == 0) == scatter
        to = mix(near[axis], far[axis], flip) if with_first else mix(far[axis], near[axis], flip)
        kept = (2 * hi, 2) if with_first else (2 * hi + lo, 1)
        given = (2 - 2 * hi, 2) if with_first else (2 * hi + 1 - lo, 1)
        if scatter:
            src = turn.at[pl.ds(m, 1)] if t == 5 else units(m, colour, flip, stage, *given)
            return src, land(m, stage, step), land(m, stage, step), to, kept
        src = units(m, colour, flip, stage, *kept)
        return src, src, units(m, colour, flip, stage, *given), to, given

    def message(t, m, colour, flip):
        src, dst, _, to, _ = copies(t, m, colour, flip)
        return remote(src, dst, ring_send.at[m], ring_recv.at[m, t], to)

    def arrival(t, m, colour, flip):
        _, _, here, to, _ = copies(t, m, colour, flip)
        return remote(here, here, ring_send.at[m], ring_recv.at[m, t], to)

    def pair(colour, flip, k):
        hi, _ = bits(colour, flip, 1)
        return mix(2 - 2 * hi, 2 * hi, k)

    def load_copy(g_ref, m, layer, colour, flip, k):
        blocks = pl.ds(own + pair(colour, flip, k), 2)
        return pltpu.make_async_copy(g_ref.at[layer, blocks], work.at[m, blocks], load_sem.at[m, k])

    def swap_copy(g_ref, m, layer, colour, flip, k):
        first = pair(colour, flip, k)
        return remote(g_ref.at[layer, pl.ds(other + first, 2)], land0.at[m, pl.ds(first, 2)], d0_send.at[m, k], d0_recv.at[m, k], partner)

    def final(colour, flip, k):
        hi, lo = bits(colour, flip, 1)
        return ((2 * hi + lo, 1), (2 * hi + 1 - lo, 1), (2 - 2 * hi, 2))[k]

    def share_copy(m, colour, flip, k, half):
        first, count = final(colour, flip, k)
        blocks = work.at[m, pl.ds(half + first, count)]
        return remote(blocks, blocks, d1_send.at[m, k], d1_recv.at[m, k], partner)

    def out_copy(o_ref, m, layer, colour, flip, k, half, slot):
        first, count = final(colour, flip, k)
        blocks = pl.ds(half + first, count)
        return pltpu.make_async_copy(work.at[m, blocks], o_ref.at[layer, blocks], out_sem.at[m, slot])

    def accumulate(dst, sources):
        for block in range(dst.shape[0]):
            if len(sources) == 2:
                dst[block] = sources[0][block] + sources[1][block]
            else:
                total = sources[0][block].astype(F32)
                for source in sources[1:]:
                    total = total + source[block].astype(F32)
                dst[block] = total.astype(BF16)

    head_way = 1 - 2 * core

    def head_message(j, back):
        axis, s = divmod(j, n - 1)
        index = lax.rem(pos[axis] - head_way * (s + back) + 2 * n, n)
        to = me + (lax.rem(pos[axis] + head_way + n, n) - pos[axis]) * strides[axis]
        if axis == 0:
            part = head.at[core, pos[2], pos[1], index]
        elif axis == 1:
            part = head.at[core, pos[2], index]
        else:
            part = head.at[core, index]
        return remote(part, part, head_send, head_recv.at[j], to)

    def head_share(which):
        return remote(head.at[which], head.at[which], head_send, head_recv.at[3 * (n - 1)], partner)

    def head_tick(t):
        count = 3 * (n - 1)
        if t == 0:
            first = pltpu.make_async_copy(head_ref, head.at[core, pos[2], pos[1], pos[0]], head_sem)
            first.start()
            first.wait()
        elif t <= count:
            head_message(t - 1, 1).wait_recv()
            head_message(t - 1, 0).wait_send()
        if t < count:
            head_message(t, 0).start()
        elif t == count:
            head_share(core).start()

    for k in range(2):
        def begin(g_ref, o_ref, m, layer, colour, flip, k=k):
            swap_copy(g_ref, m, layer, colour, flip, k).start()
            load_copy(g_ref, m, layer, colour, flip, k).start()
        each(begin)

    for t in range(13):
        def tick(g_ref, o_ref, m, layer, colour, flip, t=t):
            if t > 0:
                arrival(t - 1, m, colour, flip).wait_recv()
                message(t - 1, m, colour, flip).wait_send()
            if t < 2:
                load_copy(g_ref, m, layer, colour, flip, t).wait()
                swap_copy(g_ref, m, layer, colour, flip, t).wait_recv()
                blocks = units(m, colour, flip, 1, pair(colour, flip, t), 2)
                sources = [land0.at[m, pl.ds(pair(colour, flip, t), 2)]] + ([land(m, 1, 0)] if t > 0 else [])
                accumulate(blocks, [blocks] + sources)
            elif t == 5:
                hi, lo = bits(colour, flip, 3)
                mine, theirs = units(m, colour, flip, 3, 2 * hi + lo, 1), units(m, colour, flip, 3, 2 * hi + 1 - lo, 1)
                accumulate(turn.at[pl.ds(m, 1)], [theirs, land_unit(m, 1 - lo)])
                accumulate(mine, [mine, land_unit(m, lo)])
            elif t < 7:
                _, _, here, _, kept = copies(t - 1, m, colour, flip)
                blocks = units(m, colour, flip, (t + 1) // 2, *kept)
                accumulate(blocks, [blocks, here])
            if t < 12:
                message(t, m, colour, flip).start()
            k = t - 10
            if k >= 0:
                share_copy(m, colour, flip, k, own).start()
                out_copy(o_ref, m, layer, colour, flip, k, own, k).start()
            if k >= 1:
                share_copy(m, colour, flip, k - 1, other).wait_recv()
                out_copy(o_ref, m, layer, colour, flip, k - 1, other, k + 2).start()
        each(tick)
        head_tick(t)

    head_share(1 - core).wait_recv()
    head_share(core).wait_send()
    head_out = pltpu.make_async_copy(head, all_ref, head_sem)
    head_out.start()

    def finish(g_ref, o_ref, m, layer, colour, flip):
        share_copy(m, colour, flip, 2, other).wait_recv()
        out_copy(o_ref, m, layer, colour, flip, 2, other, 5).start()
    each(finish)

    def drain(g_ref, o_ref, m, layer, colour, flip):
        for k in range(3):
            share_copy(m, colour, flip, k, own).wait_send()
            out_copy(o_ref, m, layer, colour, flip, k, own, k).wait()
            out_copy(o_ref, m, layer, colour, flip, k, other, k + 3).wait()
        for k in range(2):
            swap_copy(g_ref, m, layer, colour, flip, k).wait_send()
    each(drain)
    head_out.wait()


def sum_gradients(g1, g2, head_part, group_size):
    n = RING
    if group_size != 2 * n ** 3:
        raise ValueError("needs a 4x4x4 torus")
    layers, blocks, rows, lanes = g1.shape
    count = 2 * layers
    dma = pltpu.SemaphoreType.DMA
    head_shape = (2, n, n, n) + head_part.shape
    return pl.pallas_call(
        functools.partial(sum_body, layers),
        in_specs=[pl.BlockSpec(memory_space=pl.ANY)] * 3,
        out_specs=[pl.BlockSpec(memory_space=pl.ANY)] * 3,
        out_shape=[
            jax.ShapeDtypeStruct(g1.shape, BF16),
            jax.ShapeDtypeStruct(g2.shape, BF16),
            jax.ShapeDtypeStruct(head_shape, BF16),
        ],
        scratch_shapes=[
            pltpu.VMEM((count, blocks, rows, lanes), BF16),
            pltpu.VMEM((count, n, rows, lanes), BF16),
            pltpu.VMEM((count, 3, rows, lanes), BF16),
            pltpu.VMEM((count, 3 * rows // n, lanes), BF16),
            pltpu.VMEM((count, 3 * rows // (n * n), lanes), BF16),
            pltpu.VMEM((count, rows // (n * n), lanes), BF16),
            pltpu.VMEM(head_shape, BF16),
            dma((count, 2)),
            dma((count, 2)),
            dma((count, 2)),
            dma((count,)),
            dma((count, 12)),
            dma((count, 3)),
            dma((count, 3)),
            dma((count, 6)),
            dma,
            dma((3 * (n - 1) + 1,)),
            dma,
        ],
        cost_estimate=cost(1 << 30, 4 * g1.size),
        compiler_params=pltpu.CompilerParams(collective_id=0, has_side_effects=True, vmem_limit_bytes=60 << 20),
        name="gradient_sum",
    )(g1, g2, head_part)


def head_backward(pooled, lab_row, w_head_b, examples):
    logits = jnp.dot(pooled, w_head_b, preferred_element_type=F32)
    soft_prob = jax.nn.softmax(logits, axis=-1)
    onehot = (lab_row[:, None] == jnp.arange(logits.shape[1])[None, :]).astype(F32)
    d_logits = ((soft_prob - onehot) / examples).astype(BF16)
    d_pooled = jnp.einsum('bc,dc->bd', d_logits, w_head_b, preferred_element_type=F32)
    return d_logits, d_pooled


def solution(mesh):
    group_size = mesh.shape['data']

    def local_step(x_step, labels, x_next, w_in, w_out, w_head, mom_in, mom_out, mom_head, learn_rate, mom_coef):
        micro_count, images, seq, d = x_step.shape
        layers = w_in.shape[0]
        classes = w_head.shape[1]
        batch = micro_count * images
        examples = batch * group_size
        xs, pre, sums = forward(x_step.reshape(-1, d), batch, w_in, w_out)
        pooled = (sums[:batch] / seq).astype(BF16)
        d_logits, d_pooled = head_backward(pooled, labels.reshape(-1), w_head.astype(BF16), examples)
        wide = -(-classes // 512) * 512
        head_part = jnp.concatenate([pooled, jnp.pad(d_logits, ((0, 0), (0, wide - classes)))], axis=1)
        d_top = jnp.pad(d_pooled / seq, ((0, 8 - batch), (0, 0)))
        g_in, g_out = backward(d_top, batch, xs, pre, w_in, w_out, layers - 1, layers)
        block_shape = (layers, -1) + g_out.shape[3:]
        red_in, red_out, head_all = sum_gradients(g_in, g_out.reshape(block_shape), head_part.reshape(16, -1), group_size)
        coef = jnp.stack([learn_rate, mom_coef])
        new_w_in, new_mom_in, new_w_out, new_mom_out, next_sums = update_forward(coef, x_next.reshape(-1, d), images, w_in, mom_in, red_in, w_out, mom_out, red_out.reshape(g_out.shape))
        head_rows = head_all.reshape(examples, d + wide)
        g_head = jnp.einsum('bd,bc->dc', head_rows[:, :d], head_rows[:, d:d + classes], preferred_element_type=F32)
        new_mom_head = mom_coef * mom_head + g_head
        new_w_head = w_head - learn_rate * new_mom_head
        next_pooled = (next_sums[:images] / seq).astype(BF16)
        logits_next = jnp.dot(next_pooled, new_w_head.astype(BF16), preferred_element_type=F32)
        return (logits_next, new_w_in, new_w_out, new_w_head, new_mom_in, new_mom_out, new_mom_head)

    return jax.shard_map(local_step, mesh=mesh, in_specs=(P(None, 'data', None, None), P(None, 'data'), P('data', None, None), P(), P(), P(), P(), P(), P(), P(), P()), out_specs=(P('data', None), P(), P(), P(), P(), P(), P()), check_vma=False)
```
